128 devices in a mesh: dev: 8 (over z_hi, y), ma: 16 (over z_lo, x, core).
Axes of the slice: x: 4, y: 4, z: 4 (z_hi: 2, z_lo: 2; z = z_hi * 2 + z_lo), core: 2. Of those that a mesh axis runs over, the one named last changes fastest.
Arguments:
- joined_weight: bfloat16 [8, 4096, 6144], P(None, 'dev', 'ma'), may hold values from -6 to 6
- norm_gain: float32 [8, 4096], P(None, 'ma'), may hold values from 0.5 to 1.5
- rotary_order: int32 [128], replicated, may hold values from 0 to 127, each once
Outputs:
- query_weight: bfloat16 [8, 4096, 4096], P(None, 'dev', 'ma')
- key_weight: bfloat16 [8, 1024, 4096], P(None, 'dev', 'ma')
- value_weight: bfloat16 [8, 1024, 4096], P(None, 'dev', 'ma')
- row_peak: float32 [8, 6144], P(None, 'dev')
The draws below stay inside these ranges and needn't reach their ends.
Inputs may be any that keep to these rules, and one draw needn't show every extreme that they name: rotary_order holds every number of 0 to 127 exactly once.
All inputs are finite; a program needn't handle non-finite values.
Results may differ from the reference program's by a relative error of at most 0.0055.
Values may be sent and summed in bfloat16 or wider, within the bound.
A program may use at most 128 MiB of HBM per device.

```python
import jax
import jax.numpy as jnp

D = 4096
HEADS = 32
KV_HEADS = 8
HEAD_DIM = 128
LAYERS = 8
GROUP = 4
QKV_COLS = 6144


def shard_levels(stream_key, shape, pieces, low, top_value):
    def one(position, parts):
        steps = jax.random.uniform(jax.random.fold_in(jax.random.fold_in(stream_key, 6), position), (parts,), jnp.float32, low / len(pieces), top_value / len(pieces))
        return jnp.repeat(jnp.exp(steps), shape[position] // parts).reshape((-1,) + (1,) * (len(shape) - position - 1))

    level = one(*pieces[0])
    for cut in pieces[1:]:
        level = level * one(*cut)
    return level


def bell_draw(stream_key, extent, width, reach, cuts=(), kind=jnp.bfloat16):
    drawn = jax.random.normal(stream_key, extent, jnp.float32) * width
    if len(cuts) > 0:
        drawn = shard_levels(stream_key, extent, cuts, -0.22, 0.18) * drawn
    return jnp.clip(drawn, min=-reach, max=reach).astype(kind)


def setup_inputs(seed: int = 0) -> dict:
    keys = jax.random.split(jax.random.key(seed), 4)
    return {
        "joined_weight": bell_draw(keys[0], (LAYERS, D, QKV_COLS), 1.0, 6.0, ((1, 8), (2, 16))),
        "norm_gain": jnp.clip(1.0 + 0.1 * jax.random.normal(keys[1], (LAYERS, D), jnp.float32), 0.5, 1.5),
        "rotary_order": jax.random.permutation(keys[2], HEAD_DIM).astype(jnp.int32),
    }


def arrange_whole(stored_layer):
    head_total = HEADS + 2 * KV_HEADS
    split = stored_layer.reshape(1, D, HEAD_DIM, head_total)
    slots_query = split[..., :HEADS].reshape(1, D, HEAD_DIM, KV_HEADS, GROUP)
    slots_key = split[..., HEADS:HEADS + KV_HEADS][..., None]
    slots_value = split[..., HEADS + KV_HEADS:][..., None]
    grouped = jnp.concatenate([slots_query, slots_key, slots_value], axis=4)
    return jnp.transpose(grouped, (0, 3, 4, 2, 1))


def finish_tiles(canonical, gain_rows, rotary_order):
    layer_count = canonical.shape[0]
    column_count = canonical.shape[4]
    turned = jnp.take(canonical[:, :, :GROUP + 1], rotary_order, axis=3)
    complete = jnp.concatenate([turned, canonical[:, :, GROUP + 1:]], axis=2)
    scaled = (complete.astype(jnp.float32) * gain_rows[:, None, None, None, :]).astype(jnp.bfloat16)
    query_rows = scaled[:, :, :GROUP].reshape(layer_count, -1, column_count)
    key_rows = scaled[:, :, GROUP].reshape(layer_count, -1, column_count)
    value_rows = scaled[:, :, GROUP + 1].reshape(layer_count, -1, column_count)
    local_peak = jnp.max(jnp.abs(scaled.astype(jnp.float32)), axis=4).reshape(layer_count, -1)
    return query_rows, key_rows, value_rows, local_peak


def reference(joined_weight, norm_gain, rotary_order):
    collected = []
    for layer_index in range(LAYERS):
        canonical = arrange_whole(joined_weight[layer_index])
        gain_rows = norm_gain[layer_index:layer_index + 1]
        collected.append(finish_tiles(canonical, gain_rows, rotary_order))
    query_weight = jnp.concatenate([item[0] for item in collected], axis=0)
    key_weight = jnp.concatenate([item[1] for item in collected], axis=0)
    value_weight = jnp.concatenate([item[2] for item in collected], axis=0)
    row_peak = jnp.concatenate([item[3] for item in collected], axis=0)
    return query_weight, key_weight, value_weight, row_peak
```

```python
import jax
import jax.numpy as jnp
from jax import lax
from jax.experimental import pallas as pl
from jax.experimental.pallas import tpu as pltpu
from jax.sharding import PartitionSpec as P

LAYERS = 8
CHUNKS = 16
FEATS = 256
COLS = 384
PIECE = 48
EARLY = 6
LAG_SWAP, LAG_X, LAG_Z, LAG_F = 3, 4, 6, 8
MESH = pl.DeviceIdType.MESH


def sort_matrix(pm_ref):
    row = lax.broadcasted_iota(jnp.int32, (COLS, 128), 0)
    lane = lax.broadcasted_iota(jnp.int32, (COLS, 128), 1)
    g = (row * 1366) >> 16
    rest = row - g * PIECE
    s, dd = rest >> 3, rest & 7
    head = jnp.where(s < 4, g * 4 + s, 32 + (s - 4) * 8 + g)
    column = dd * PIECE + head
    for block in range(COLS // 128):
        pm_ref[:, block * 128 : (block + 1) * 128] = jnp.where(column == lane + block * 128, 1.0, 0.0).astype(jnp.bfloat16)


def order_matrix(rot_ref, rm_ref, zl):
    spread = jnp.broadcast_to(rot_ref[0:1, :], (128, 128))
    turned = jnp.transpose(spread)
    plain = lax.broadcasted_iota(jnp.int32, (128, 128), 0)
    lane = lax.broadcasted_iota(jnp.int32, (128, 128), 1)
    for s in range(6):
        stored = turned if s < 5 else plain
        piece = stored >> 3
        half = piece >> 3
        slot = jnp.where(zl == 1, half, 1 - half)
        column = slot * COLS + (piece & 7) * PIECE + s * 8 + (stored & 7)
        for block in range(2 * COLS // 128):
            rm_ref[s * 128 : (s + 1) * 128, block * 128 : (block + 1) * 128] = jnp.where(
                column == lane + block * 128, 1.0, 0.0
            ).astype(jnp.bfloat16)


def kernel(
    rot_ref, gain_ref, w_ref, q_ref, k_ref, v_ref, peak_ref,
    xb, sb, yb, gb, ob, pk, pm, rm,
    in_sem, swap_sem, y_sem, x_sem, z_sem, swap_out, y_out, x_out, z_out, o_sem, pk_sem, pk_out,
):
    dev, ma = lax.axis_index("dev"), lax.axis_index("ma")
    zh, y = dev // 4, dev % 4
    zl, x, c = ma // 8, (ma // 2) % 4, ma % 2
    z = zh * 2 + zl
    mid = (z == 1) | (z == 2)
    end = (z == 0) | (z == 3)

    def at(x_, y_, z_, c_):
        return {"dev": (z_ // 2) * 4 + y_, "ma": (z_ % 2) * 8 + x_ * 2 + c_}

    def send(src, dst, out_sem, in_sem_, device):
        pltpu.make_async_remote_copy(src, dst, out_sem, in_sem_, device_id=device, device_id_type=MESH).start()

    def done(ref, sem):
        pltpu.make_async_copy(ref, ref, sem).wait()

    def load(t):
        return pltpu.make_async_copy(w_ref.at[t // 2, pl.ds((t % 2) * FEATS, FEATS), :], xb.at[t], in_sem.at[t])

    for t in range(CHUNKS):
        load(t).start()

    barrier = pltpu.get_barrier_semaphore()
    for step in range(1, 4):
        pl.semaphore_signal(barrier, inc=1, device_id=at(x, (y + step) % 4, z, c), device_id_type=MESH)
    for step in range(1, 16):
        pl.semaphore_signal(barrier, inc=1, device_id={"dev": dev, "ma": (ma + step) % 16}, device_id_type=MESH)
    pl.semaphore_signal(barrier, inc=1, device_id=at(x, y, 3 - z, c), device_id_type=MESH)

    sort_matrix(pm)
    order_matrix(rot_ref, rm, zl)
    pl.semaphore_wait(barrier, 19)

    def along_y(t, q):
        pltpu.make_async_copy(sb.at[t, q, y], yb.at[t, q, y], y_sem.at[t * 2 + q]).start()
        for step in (2, 1, 3):
            far = (y + step) % 4
            send(sb.at[t, q, far], yb.at[t, q, y], y_out.at[t], y_sem.at[t * 2 + q], at(x, far, z, c))

    def sort(t):
        load(t).wait()
        for half in range(2):
            rows = lax.dot_general(
                pm[half * 192 : (half + 1) * 192, :], xb[t], (((1,), (1,)), ((), ())), preferred_element_type=jnp.float32
            )
            place = jnp.where(zh == half, 0, jnp.where(mid, 1, 2))
            sb[t, place] = rows.astype(jnp.bfloat16).reshape(4, PIECE, FEATS)

    def first_sends(t):
        @pl.when(end)
        def _():
            send(sb.at[t, 2], sb.at[t, 1], swap_out.at[t], swap_sem.at[t], at(x, y, 3 - z, c))

        along_y(t, 0)

        @pl.when(mid)
        def _():
            along_y(t, 1)

    def swapped(t):
        @pl.when(end)
        def _():
            done(sb.at[t, 1], swap_sem.at[t])
            along_y(t, 1)

    def along_x(t):
        layer, core = t // 2, t % 2
        for q in range(2):
            done(yb.at[t, q], y_sem.at[t * 2 + q])
            slot = jnp.where(end, 1, 2) if q == 0 else 3
            place = gb.at[layer, slot, x * 2 + c]
            for step in (2, 1, 3):
                far = (x + step) % 4
                send(yb.at[t, q, far], place, x_out.at[t], x_sem.at[layer * 2 + q], at(far, y, z, core))

            @pl.when(core != c)
            def _():
                send(yb.at[t, q, x], place, x_out.at[t], x_sem.at[layer * 2 + q], at(x, y, z, 1 - c))

            @pl.when(core == c)
            def _():
                pltpu.make_async_copy(yb.at[t, q, x], place, x_sem.at[layer * 2 + q]).start()

    def along_z(layer):
        done(gb.at[layer, 2], x_sem.at[layer * 2])

        @pl.when(mid)
        def _():
            send(gb.at[layer, 2], gb.at[layer, 0], z_out.at[layer], z_sem.at[layer * 2], at(x, y, 3 * (z // 2), c))

        done(gb.at[layer, 3], x_sem.at[layer * 2 + 1])
        slot = jnp.where(end, 1, 0)
        send(gb.at[layer, 3], gb.at[layer, slot], z_out.at[layer], z_sem.at[layer * 2 + slot], at(x, y, 1 + z % 2, c))

    def send_peaks(part, first, count):
        for step in range(1, 16):
            block = pk.at[ma, pl.ds(first, count)]
            send(block, block, pk_out.at[part], pk_sem.at[part], {"dev": dev, "ma": (ma + step) % 16})

    def finish(layer):
        done(gb.at[layer, 0], z_sem.at[layer * 2])

        @pl.when(mid)
        def _():
            done(gb.at[layer, 1], z_sem.at[layer * 2 + 1])

        arrived = gb[layer, 0:2].reshape(2 * COLS, FEATS)
        gain = gain_ref[pl.ds(layer, 1), :]
        for s in range(6):
            rows = jnp.dot(rm[s * 128 : (s + 1) * 128, :], arrived, preferred_element_type=jnp.float32) * gain
            ob[layer, s * 128 : (s + 1) * 128, :] = rows.astype(jnp.bfloat16)
            size = jnp.abs(rows)
            size = jnp.transpose(jnp.maximum(size[:, :128], size[:, 128:]))
            top = jnp.max(size, axis=0, keepdims=True)
            pk[ma, layer, s : s + 1, :] = top.astype(jnp.bfloat16).astype(jnp.float32)
        pltpu.make_async_copy(ob.at[layer, pl.ds(0, 512)], q_ref.at[layer], o_sem.at[layer]).start()
        pltpu.make_async_copy(ob.at[layer, pl.ds(512, 128)], k_ref.at[layer], o_sem.at[layer]).start()
        pltpu.make_async_copy(ob.at[layer, pl.ds(640, 128)], v_ref.at[layer], o_sem.at[layer]).start()

        @pl.when(layer == EARLY - 1)
        def _():
            send_peaks(0, 0, EARLY)

        @pl.when(layer == LAYERS - 1)
        def _():
            send_peaks(1, EARLY, LAYERS - EARLY)

    def turn(i, carry):
        def during(lag, stage):
            t = i - lag

            @pl.when((t >= 0) & (t < CHUNKS))
            def _():
                stage(t)

        def mine(stage):
            def run(t):
                @pl.when(t % 2 == c)
                def _():
                    stage(t // 2)

            return run

        during(0, sort)
        during(1, first_sends)
        during(LAG_SWAP, swapped)
        during(LAG_X, along_x)
        during(LAG_Z, mine(along_z))
        during(LAG_F, mine(finish))
        return carry

    lax.fori_loop(0, CHUNKS + LAG_F, turn, 0)

    def close(t, carry):
        done(sb.at[t, 0:2, 0:3], y_out.at[t])

        @pl.when(end)
        def _():
            done(sb.at[t, 2], swap_out.at[t])

        @pl.when(t % 2 == c)
        def _():
            done(yb.at[t, :, 0:3], x_out.at[t])

        @pl.when(t % 2 != c)
        def _():
            done(yb.at[t], x_out.at[t])

        return carry

    lax.fori_loop(0, CHUNKS, close, 0)

    def close_layer(layer, carry):
        @pl.when(end)
        def _():
            done(gb.at[layer, 3], z_out.at[layer])

        @pl.when(mid)
        def _():
            done(gb.at[layer, 2:4], z_out.at[layer])

        done(ob.at[layer], o_sem.at[layer])
        return carry

    lax.fori_loop(0, LAYERS, close_layer, 0)

    for part, count in ((0, EARLY), (1, LAYERS - EARLY)):
        done(pk.at[0:15, 0:count], pk_sem.at[part])
        done(pk.at[0:15, 0:count], pk_out.at[part])
    for s in range(6):
        peak_ref[:, s * 128 : (s + 1) * 128] = jnp.max(pk[:, :, s, :], axis=0)


def shards(joined_weight, norm_gain, rotary_order):
    dma = pltpu.SemaphoreType.DMA
    bf16 = jnp.bfloat16
    return pl.pallas_call(
        kernel,
        name="relayout",
        out_shape=(
            jax.ShapeDtypeStruct((LAYERS, 512, FEATS), bf16),
            jax.ShapeDtypeStruct((LAYERS, 128, FEATS), bf16),
            jax.ShapeDtypeStruct((LAYERS, 128, FEATS), bf16),
            jax.ShapeDtypeStruct((LAYERS, 768), jnp.float32),
        ),
        in_specs=[
            pl.BlockSpec(memory_space=pltpu.VMEM),
            pl.BlockSpec(memory_space=pltpu.VMEM),
            pl.BlockSpec(memory_space=pl.ANY),
        ],
        out_specs=(
            pl.BlockSpec(memory_space=pl.ANY),
            pl.BlockSpec(memory_space=pl.ANY),
            pl.BlockSpec(memory_space=pl.ANY),
            pl.BlockSpec(memory_space=pltpu.VMEM),
        ),
        scratch_shapes=[
            pltpu.VMEM((CHUNKS, FEATS, COLS), bf16),
            pltpu.VMEM((CHUNKS, 3, 4, PIECE, FEATS), bf16),
            pltpu.VMEM((CHUNKS, 2, 4, PIECE, FEATS), bf16),
            pltpu.VMEM((LAYERS, 4, 8, PIECE, FEATS), bf16),
            pltpu.VMEM((LAYERS, 768, FEATS), bf16),
            pltpu.VMEM((16, LAYERS, 8, 128), jnp.float32),
            pltpu.VMEM((COLS, COLS), bf16),
            pltpu.VMEM((768, 768), bf16),
            dma((CHUNKS,)),
            dma((CHUNKS,)),
            dma((CHUNKS * 2,)),
            dma((LAYERS * 2,)),
            dma((LAYERS * 2,)),
            dma((CHUNKS,)),
            dma((CHUNKS,)),
            dma((CHUNKS,)),
            dma((LAYERS,)),
            dma((LAYERS,)),
            dma((2,)),
            dma((2,)),
        ],
        compiler_params=pltpu.CompilerParams(collective_id=0, has_side_effects=True, vmem_limit_bytes=40 * 2**20),
    )(rotary_order.reshape(1, 128), norm_gain, joined_weight)


def solution(mesh):
    placed = (P(None, "dev", "ma"), P(None, "ma"), P())
    tiles = P(None, "dev", "ma")
    return jax.shard_map(shards, mesh=mesh, in_specs=placed, out_specs=(tiles, tiles, tiles, P(None, "dev")), check_vma=False)
```

```python
import jax
import jax.numpy as jnp
from jax import lax
from jax.experimental import pallas as pl
from jax.experimental.pallas import tpu as pltpu
from jax.sharding import PartitionSpec as P

LAYERS = 8
CHUNKS = 16
FEATS = 256
COLS = 384
PIECE = 48
PAIRS = 3
AHEAD = 4
SKEW = 3
STEPS = 2 * CHUNKS
LAG_X, LAG_Z, LAG_F = 4, 8, 12
PEAKS_FROM, PEAKS_SEND, PEAKS_GROUP, PEAKS_SPREAD, PEAKS_LAST = 8, 24, 28, 30, 36
MESH = pl.DeviceIdType.MESH


def sort_matrix(pm_ref):
    row = lax.broadcasted_iota(jnp.int32, (COLS, 128), 0)
    lane = lax.broadcasted_iota(jnp.int32, (COLS, 128), 1)
    g = (row * 1366) >> 16
    rest = row - g * PIECE
    s, dd = rest >> 3, rest & 7
    head = jnp.where(s < 4, g * 4 + s, 32 + (s - 4) * 8 + g)
    column = dd * PIECE + head
    for block in range(COLS // 128):
        pm_ref[:, block * 128 : (block + 1) * 128] = jnp.where(column == lane + block * 128, 1.0, 0.0).astype(jnp.bfloat16)


def order_matrix(rot_ref, rm_ref, zl):
    turned = jnp.transpose(jnp.broadcast_to(rot_ref[0:1, :], (128, 128)))
    plain = lax.broadcasted_iota(jnp.int32, (128, 128), 0)
    lane = lax.broadcasted_iota(jnp.int32, (128, 128), 1)

    def hot(stored, s2, block):
        piece = stored >> 3
        half = piece >> 3
        slot = jnp.where(zl == 1, half, 1 - half)
        column = slot * 128 + (piece & 7) * 16 + s2 * 8 + (stored & 7)
        return jnp.where(column == lane + block * 128, 1.0, 0.0).astype(jnp.bfloat16)

    for block in range(2):
        lanes = slice(block * 128, (block + 1) * 128)
        key = hot(turned, 0, block)
        rm_ref[0, 0:128, lanes] = key
        rm_ref[1, 0:128, lanes] = key
        rm_ref[0, 128:256, lanes] = hot(turned, 1, block)
        rm_ref[1, 128:256, lanes] = hot(plain, 1, block)


def kernel(
    rot_ref, gain_ref, w_ref, out_ref, peak_ref,
    rv, gv, gs, xb, sb, yb, gb, ob, pt, pk1, pk2, pm, rm,
    in_sem, rot_sem, gain_sem, gs_sem, gs_out, swap_sem, y_sem, x_sem, z_sem, swap_out, y_out, x_out, z_out, o_sem,
    pk1_sem, pk1_out, pk2_sem, pk2_out,
):
    dev, ma = lax.axis_index("dev"), lax.axis_index("ma")
    zh, y = dev // 4, dev % 4
    zl, x, c = ma // 8, (ma // 2) % 4, ma % 2
    z = zh * 2 + zl
    inner = (z == 1) | (z == 2)
    outer = (z == 0) | (z == 3)
    opposite = {"dev": (1 - zh) * 4 + y, "ma": (1 - zl) * 8 + x * 2 + c}

    def at(x_, y_, z_, c_):
        return {"dev": (z_ // 2) * 4 + y_, "ma": (z_ % 2) * 8 + x_ * 2 + c_}

    def send(src, dst, out_sem, in_sem_, device):
        pltpu.make_async_remote_copy(src, dst, out_sem, in_sem_, device_id=device, device_id_type=MESH).start()

    def done(ref, sem):
        pltpu.make_async_copy(ref, ref, sem).wait()

    def load(t):
        return pltpu.make_async_copy(w_ref.at[t // 2, pl.ds((t % 2) * FEATS, FEATS), :], xb.at[t], in_sem.at[t])

    load_rot = pltpu.make_async_copy(rot_ref, rv, rot_sem)
    load_gain = pltpu.make_async_copy(gain_ref, gv, gain_sem)

    for t in range(CHUNKS):
        load(t).start()
    load_rot.start()
    load_gain.start()

    barrier = pltpu.get_barrier_semaphore()
    for step in range(1, 16):
        pl.semaphore_signal(barrier, inc=1, device_id={"dev": dev, "ma": (ma + step) % 16}, device_id_type=MESH)
    for step in range(1, 8):
        pl.semaphore_signal(barrier, inc=1, device_id={"dev": (dev + step) % 8, "ma": ma}, device_id_type=MESH)
    pl.semaphore_signal(barrier, inc=1, device_id=opposite, device_id_type=MESH)

    def place(half):
        return jnp.where(zh == half, 0, jnp.where(inner, 1, 2))

    def sort(t):
        load(t).wait()
        rows = lax.dot_general(pm[...], xb[t], (((1,), (1,)), ((), ())), preferred_element_type=jnp.float32)
        rows = rows.astype(jnp.bfloat16).reshape(2, 4, PAIRS, 16, FEATS)
        sb[t, place(0)] = rows[0]
        sb[t, place(1)] = rows[1]

    def swap(t):
        @pl.when(outer)
        def _():
            send(sb.at[t, 2], sb.at[t, 1], swap_out.at[t], swap_sem.at[t], opposite)

    sort_matrix(pm)
    for t in range(AHEAD):
        sort(t)
    load_gain.wait()
    load_rot.wait()
    pl.semaphore_wait(barrier, 23)
    for t in range(AHEAD):
        swap(t)

    def along_y(t, q):
        @pl.when(outer & (q == 1))
        def _():
            done(sb.at[t, 1], swap_sem.at[t])

        pltpu.make_async_copy(sb.at[t, q, y], yb.at[t, q, y], y_sem.at[t * 2 + q]).start()
        for step in (2, 1, 3):
            far = (y + step) % 4
            send(sb.at[t, q, far], yb.at[t, q, y], y_out.at[t], y_sem.at[t * 2 + q], at(x, far, z, c))

    def along_x(t, q):
        layer, core = t // 2, t % 2
        arrived, sem = x_out.at[t], x_sem.at[layer * 2 + q]
        done(yb.at[t, q], y_sem.at[t * 2 + q])
        slot = jnp.where(q == 1, 3, jnp.where(outer, 1, 2))
        target = gb.at[layer, :, slot, x * 2 + c]
        for step in (2, 1, 3):
            far = (x + step) % 4
            send(yb.at[t, q, far], target, arrived, sem, at(far, y, z, core))

        @pl.when(core != c)
        def _():
            send(yb.at[t, q, x], target, arrived, sem, at(x, y, z, 1 - c))

        @pl.when(core == c)
        def _():
            pltpu.make_async_copy(yb.at[t, q, x], target, sem).start()

    def along_z(t, q):
        layer = t // 2

        @pl.when(t % 2 == c)
        def _():
            done(gb.at[layer, :, 2 + q], x_sem.at[layer * 2 + q])

            @pl.when(inner | (q == 1))
            def _():
                slot = jnp.where(outer, 1, 0)
                to = jnp.where(q == 1, 1 + z % 2, 3 * (z // 2))
                target = gb.at[layer, :, slot]
                send(gb.at[layer, :, 2 + q], target, z_out.at[layer], z_sem.at[layer * 2 + slot], at(x, y, to, c))

    def finish(t, q):
        layer = t // 2

        @pl.when((t % 2 == c) & ((outer & (q == 0)) | (inner & (q == 1))))
        def _():
            done(gb.at[layer, :, 0], z_sem.at[layer * 2])

            @pl.when(inner)
            def _():
                done(gb.at[layer, :, 1], z_sem.at[layer * 2 + 1])

            gain = gv[pl.ds(layer, 1), :]
            for pair in range(PAIRS):
                arrived = gb[layer, pair, 0:2].reshape(256, FEATS)
                rows = jnp.dot(rm[pair // 2], arrived, preferred_element_type=jnp.float32) * gain
                ob[layer, pair * 256 : (pair + 1) * 256, :] = rows.astype(jnp.bfloat16)
            pltpu.make_async_copy(ob.at[layer], out_ref.at[layer], o_sem.at[layer]).start()

    def share_gain():
        @pl.when(ma // 2 == dev)
        def _():
            block = ma % 2
            pltpu.make_async_copy(gv, gs.at[block], gs_sem.at[block]).start()
            for step in range(1, 16):
                send(gv, gs.at[block], gs_out, gs_sem.at[block], {"dev": dev, "ma": (ma + step) % 16})

    def peaks(layer):
        @pl.when(layer == 0)
        def _():
            done(gs.at[0], gs_sem.at[0])
            done(gs.at[1], gs_sem.at[1])

        lane = lax.broadcasted_iota(jnp.int32, (192, 128), 1)
        for half in range(2):
            size = None
            for core in range(2):
                rows = sb[layer * 2 + core, place(half)].reshape(192, FEATS).astype(jnp.float32)
                rows = jnp.abs(rows * gs[core, pl.ds(layer, 1), :])
                rows = jnp.maximum(rows[:, :128], rows[:, 128:])
                size = rows if size is None else jnp.maximum(size, rows)
            top = jnp.max(size, axis=1, keepdims=True)
            part = slice(half * 192, (half + 1) * 192)
            pt[part, :] = jnp.where(lane == layer, top, pt[part, :])

        @pl.when(layer == LAYERS - 1)
        def _():
            for block in range(3):
                lanes = slice(block * 128, (block + 1) * 128)
                pk1[dev, :, lanes] = jnp.transpose(pt[lanes, :])[0:LAYERS, :].astype(jnp.bfloat16).astype(jnp.float32)

    def send_peaks():
        for step in range(1, 8):
            send(pk1.at[dev], pk1.at[dev], pk1_out, pk1_sem, {"dev": (dev + step) % 8, "ma": ma})

    def group_peaks():
        done(pk1.at[0:7], pk1_sem)
        top = jnp.max(pk1[...], axis=0).astype(jnp.bfloat16)
        row = lax.broadcasted_iota(jnp.int32, (COLS, 128), 0)
        lane = lax.broadcasted_iota(jnp.int32, (COLS, 128), 1)
        pick = jnp.where((row - dev * PIECE == lane) & (lane < PIECE), 1.0, 0.0).astype(jnp.bfloat16)
        pk2[ma] = jnp.dot(top, pick, preferred_element_type=jnp.float32)

    def spread_peaks():
        for step in range(1, 16):
            send(pk2.at[ma], pk2.at[ma], pk2_out, pk2_sem, {"dev": dev, "ma": (ma + step) % 16})

    def last_peaks():
        done(pk2.at[0:15], pk2_sem)
        lane = lax.broadcasted_iota(jnp.int32, (LAYERS, 128), 1)
        for pair in range(PAIRS):
            halves = []
            for half in range(2):
                line = jnp.zeros((LAYERS, 128), jnp.float32)
                for piece in range(8):
                    shift = (piece - pair) * 16 % 128
                    part = pk2[half * 8 + piece]
                    part = pltpu.roll(part, shift, 1) if shift else part
                    line = jnp.where((lane >= piece * 16) & (lane < piece * 16 + 16), part, line)
                halves.append(line)
            low = jnp.where(zl == 1, halves[0], halves[1])
            high = jnp.where(zl == 1, halves[1], halves[0])
            line = jnp.concatenate([low, high], axis=1).astype(jnp.bfloat16)
            peak_ref[:, pair * 256 : (pair + 1) * 256] = lax.dot_general(
                line, rm[pair // 2], (((1,), (1,)), ((), ())), preferred_element_type=jnp.float32
            )

    def order(u):
        later = u - SKEW
        even = later % 2 == 0
        t = jnp.where(u < SKEW, u, jnp.where(u >= STEPS - SKEW, u - CHUNKS, jnp.where(even, later // 2, SKEW + later // 2)))
        q = jnp.where(u < SKEW, 0, jnp.where(u >= STEPS - SKEW, 1, jnp.where(even, 1, 0)))
        return t, q

    def turn(i, carry):
        def during(lag, stage):
            @pl.when((i >= lag) & (i < STEPS + lag))
            def _():
                stage(*order(i - lag))

        def keep_sorted(t, q):
            @pl.when((q == 0) & (t + AHEAD < CHUNKS))
            def _():
                sort(t + AHEAD)

            @pl.when((q == 0) & (t > 0) & (t + AHEAD - 1 < CHUNKS))
            def _():
                swap(t + AHEAD - 1)

        during(0, along_y)
        during(LAG_X, along_x)
        during(LAG_Z, along_z)
        during(0, keep_sorted)
        during(LAG_F, finish)

        @pl.when((i >= PEAKS_FROM) & (i < PEAKS_FROM + 2 * LAYERS) & (i % 2 == 0))
        def _():
            peaks((i - PEAKS_FROM) // 2)

        pl.when(i == PEAKS_SEND)(send_peaks)
        pl.when(i == PEAKS_GROUP)(group_peaks)
        pl.when(i == PEAKS_SPREAD)(spread_peaks)
        pl.when(i == PEAKS_LAST)(last_peaks)

        @pl.when(i == 0)
        def _():
            share_gain()
            order_matrix(rv, rm, zl)

        return carry

    lax.fori_loop(0, STEPS + LAG_F, turn, 0)

    def close(t, carry):
        done(sb.at[t, 0:2, 0:3], y_out.at[t])

        @pl.when(outer)
        def _():
            done(sb.at[t, 2], swap_out.at[t])

        @pl.when(t % 2 == c)
        def _():
            done(yb.at[t, :, 0:3], x_out.at[t])

        @pl.when(t % 2 != c)
        def _():
            done(yb.at[t], x_out.at[t])

        return carry

    lax.fori_loop(0, CHUNKS, close, 0)

    def close_layer(layer, carry):
        @pl.when(outer)
        def _():
            done(gb.at[layer, :, 3], z_out.at[layer])

        @pl.when(inner)
        def _():
            done(gb.at[layer, :, 2:4], z_out.at[layer])

        done(ob.at[layer], o_sem.at[layer])
        return carry

    lax.fori_loop(0, LAYERS, close_layer, 0)

    @pl.when(ma // 2 == dev)
    def _():
        done(gs.at[0:15], gs_out)

    done(pk1.at[0:7], pk1_out)
    done(pk2.at[0:15], pk2_out)


def write_out(tiles_ref, peak_ref, q_ref, k_ref, v_ref, row_ref, sem):
    copies = [
        pltpu.make_async_copy(tiles_ref.at[:, pl.ds(0, 512)], q_ref, sem.at[0]),
        pltpu.make_async_copy(tiles_ref.at[:, pl.ds(512, 128)], k_ref, sem.at[1]),
        pltpu.make_async_copy(tiles_ref.at[:, pl.ds(640, 128)], v_ref, sem.at[2]),
        pltpu.make_async_copy(peak_ref, row_ref, sem.at[3]),
    ]
    for copy in copies:
        copy.start()
    for copy in copies:
        copy.wait()


def shards(joined_weight, norm_gain, rotary_order):
    dma = pltpu.SemaphoreType.DMA
    bf16, f32 = jnp.bfloat16, jnp.float32
    hbm = pl.BlockSpec(memory_space=pltpu.HBM)
    anywhere = pl.BlockSpec(memory_space=pl.ANY)
    tiles, peak = pl.pallas_call(
        kernel,
        name="relayout",
        out_shape=(jax.ShapeDtypeStruct((LAYERS, 768, FEATS), bf16), jax.ShapeDtypeStruct((LAYERS, 768), f32)),
        in_specs=[hbm, hbm, hbm],
        out_specs=(anywhere, pl.BlockSpec(memory_space=pltpu.VMEM)),
        scratch_shapes=[
            pltpu.VMEM((1, 128), jnp.int32),
            pltpu.VMEM((LAYERS, FEATS), f32),
            pltpu.VMEM((15, LAYERS, FEATS), f32),
            pltpu.VMEM((CHUNKS, FEATS, COLS), bf16),
            pltpu.VMEM((CHUNKS, 3, 4, PAIRS, 16, FEATS), bf16),
            pltpu.VMEM((CHUNKS, 2, 4, PAIRS, 16, FEATS), bf16),
            pltpu.VMEM((LAYERS, PAIRS, 4, 8, 16, FEATS), bf16),
            pltpu.VMEM((LAYERS, 768, FEATS), bf16),
            pltpu.VMEM((COLS, 128), f32),
            pltpu.VMEM((8, LAYERS, COLS), f32),
            pltpu.VMEM((16, LAYERS, 128), f32),
            pltpu.VMEM((COLS, COLS), bf16),
            pltpu.VMEM((2, 256, 256), bf16),
            dma((CHUNKS,)),
            dma,
            dma,
            dma((2,)),
            dma,
            dma((CHUNKS,)),
            dma((CHUNKS * 2,)),
            dma((LAYERS * 2,)),
            dma((LAYERS * 2,)),
            dma((CHUNKS,)),
            dma((CHUNKS,)),
            dma((CHUNKS,)),
            dma((LAYERS,)),
            dma((LAYERS,)),
            dma,
            dma,
            dma,
            dma,
        ],
        compiler_params=pltpu.CompilerParams(collective_id=0, has_side_effects=True, vmem_limit_bytes=40 * 2**20),
    )(*(pltpu.with_memory_space_constraint(a, pltpu.HBM) for a in (rotary_order.reshape(1, 128), norm_gain, joined_weight)))
    return pl.pallas_call(
        write_out,
        name="write_out",
        out_shape=(
            jax.ShapeDtypeStruct((LAYERS, 512, FEATS), bf16),
            jax.ShapeDtypeStruct((LAYERS, 128, FEATS), bf16),
            jax.ShapeDtypeStruct((LAYERS, 128, FEATS), bf16),
            jax.ShapeDtypeStruct((LAYERS, 768), f32),
        ),
        in_specs=[anywhere, anywhere],
        out_specs=(hbm, hbm, hbm, hbm),
        scratch_shapes=[dma((4,))],
        compiler_params=pltpu.CompilerParams(vmem_limit_bytes=2**20),
    )(tiles, peak)


def solution(mesh):
    placed = (P(None, "dev", "ma"), P(None, "ma"), P())
    tiles = P(None, "dev", "ma")
    return jax.shard_map(shards, mesh=mesh, in_specs=placed, out_specs=(tiles, tiles, tiles, P(None, "dev")), check_vma=False)
```

```python
import jax
import jax.numpy as jnp
from jax import lax
from jax.experimental import pallas as pl
from jax.experimental.pallas import tpu as pltpu
from jax.sharding import PartitionSpec as P

LAYERS = 8
CHUNKS = 16
FEATS = 256
COLS = 384
PIECE = 48
PAIRS = 3
LATE = 8
AHEAD = 8
STEPS = 2 * CHUNKS
Z_LAST, Z_LAST_RELAY, Z_FIRST_RELAY, FINISH_LATE, FINISH = 5, 20, 3, 25, 23
PEAKS_FROM, PEAKS_SEND, PEAKS_GROUP, PEAKS_SPREAD, PEAKS_LAST = 10, 25, 29, 30, 34
END = max(FINISH, FINISH_LATE) + 15
MESH = pl.DeviceIdType.MESH


def sort_matrix(pm_ref):
    row = lax.broadcasted_iota(jnp.int32, (COLS, 128), 0)
    lane = lax.broadcasted_iota(jnp.int32, (COLS, 128), 1)
    g = (row * 1366) >> 16
    rest = row - g * PIECE
    s, dd = rest >> 3, rest & 7
    head = jnp.where(s < 4, g * 4 + s, 32 + (s - 4) * 8 + g)
    column = dd * PIECE + head
    for block in range(COLS // 128):
        pm_ref[:, block * 128 : (block + 1) * 128] = jnp.where(column == lane + block * 128, 1.0, 0.0).astype(jnp.bfloat16)


def order_matrix(rot_ref, rm_ref, zl):
    turned = jnp.transpose(jnp.broadcast_to(rot_ref[0:1, :], (128, 128)))
    plain = lax.broadcasted_iota(jnp.int32, (128, 128), 0)
    lane = lax.broadcasted_iota(jnp.int32, (128, 128), 1)

    def hot(stored, s2, block):
        piece = stored >> 3
        half = piece >> 3
        slot = jnp.where(zl == 1, half, 1 - half)
        column = slot * 128 + (piece & 7) * 16 + s2 * 8 + (stored & 7)
        return jnp.where(column == lane + block * 128, 1.0, 0.0).astype(jnp.bfloat16)

    for block in range(2):
        lanes = slice(block * 128, (block + 1) * 128)
        key = hot(turned, 0, block)
        rm_ref[0, 0:128, lanes] = key
        rm_ref[1, 0:128, lanes] = key
        rm_ref[0, 128:256, lanes] = hot(turned, 1, block)
        rm_ref[1, 128:256, lanes] = hot(plain, 1, block)


def kernel(
    rot_ref, gain_ref, w_ref, out_ref, peak_ref,
    rv, gv, gs, xb, sb, yb, gb, ob, pt, pk1, pk2, pm, rm,
    in_sem, rot_sem, gain_sem, gs_sem, gs_out, far_sem, near_sem, y_sem, x_sem, z_sem, first_out, y_out, x_out, z_out, o_sem,
    pk1_sem, pk1_out, pk2_sem, pk2_out,
):
    dev, ma = lax.axis_index("dev"), lax.axis_index("ma")
    zh, y = dev // 4, dev % 4
    zl, x, c = ma // 8, (ma // 2) % 4, ma % 2
    z = zh * 2 + zl
    inner = (z == 1) | (z == 2)
    outer = (z == 0) | (z == 3)
    far_z = {"dev": (1 - zh) * 4 + y, "ma": (1 - zl) * 8 + x * 2 + c}
    near_z = {"dev": dev, "ma": (1 - zl) * 8 + x * 2 + c}

    def at(x_, y_, z_, c_):
        return {"dev": (z_ // 2) * 4 + y_, "ma": (z_ % 2) * 8 + x_ * 2 + c_}

    def send(src, dst, out_sem, in_sem_, device):
        pltpu.make_async_remote_copy(src, dst, out_sem, in_sem_, device_id=device, device_id_type=MESH).start()

    def done(ref, sem):
        pltpu.make_async_copy(ref, ref, sem).wait()

    def load(t):
        return pltpu.make_async_copy(w_ref.at[t // 2, pl.ds((t % 2) * FEATS, FEATS), :], xb.at[t], in_sem.at[t])

    load_rot = pltpu.make_async_copy(rot_ref, rv, rot_sem)
    load_gain = pltpu.make_async_copy(gain_ref, gv, gain_sem)

    for n in range(CHUNKS):
        load(n // 2 + (n % 2) * LATE).start()
    load_rot.start()
    load_gain.start()

    barrier = pltpu.get_barrier_semaphore()
    for step in range(1, 16):
        pl.semaphore_signal(barrier, inc=1, device_id={"dev": dev, "ma": (ma + step) % 16}, device_id_type=MESH)
    for step in range(1, 8):
        pl.semaphore_signal(barrier, inc=1, device_id={"dev": (dev + step) % 8, "ma": ma}, device_id_type=MESH)
    pl.semaphore_signal(barrier, inc=1, device_id=far_z, device_id_type=MESH)

    def place(t, half):
        kept = zh == half
        early = jnp.where(kept, jnp.where(outer, 0, 3), 2)
        return jnp.where(t < LATE, jnp.where(kept, 0, 1), early)

    def sort(n):
        t = n // 2 + (n % 2) * LATE
        load(t).wait()
        rows = lax.dot_general(pm[...], xb[t], (((1,), (1,)), ((), ())), preferred_element_type=jnp.float32)
        rows = rows.astype(jnp.bfloat16).reshape(2, 4, PAIRS, 16, FEATS)
        sb[t, place(t, 0)] = rows[0]
        sb[t, place(t, 1)] = rows[1]

    def z_first(t):
        send(sb.at[t, 2], sb.at[t, jnp.where(outer, 3, 0)], first_out.at[t], far_sem.at[t], far_z)

        @pl.when(inner)
        def _():
            send(sb.at[t, 3], sb.at[t, 1], first_out.at[t], near_sem.at[t], near_z)

    def z_first_relay(t):
        @pl.when(outer)
        def _():
            done(sb.at[t, 3], far_sem.at[t])
            send(sb.at[t, 3], sb.at[t, 1], first_out.at[t], near_sem.at[t], near_z)

    def along_y(t, q):
        @pl.when((t >= LATE) & (q == 0) & inner)
        def _():
            done(sb.at[t, 0], far_sem.at[t])

        @pl.when((t >= LATE) & (q == 1))
        def _():
            done(sb.at[t, 1], near_sem.at[t])

        pltpu.make_async_copy(sb.at[t, q, y], yb.at[t, q, y], y_sem.at[t * 2 + q]).start()
        for step in (2, 1, 3):
            far = (y + step) % 4
            send(sb.at[t, q, far], yb.at[t, q, y], y_out.at[t], y_sem.at[t * 2 + q], at(x, far, z, c))

    def along_x(t, q):
        layer, core = t // 2, t % 2
        sent, sem = x_out.at[t], x_sem.at[layer * 2 + q]
        done(yb.at[t, q], y_sem.at[t * 2 + q])
        late = jnp.where(q == 1, 3, jnp.where(outer, 1, 2))
        slot = jnp.where(t < LATE, late, jnp.where(outer, 1 - q, q))
        target = gb.at[layer, slot, x * 2 + c]
        for step in (2, 1, 3):
            far = (x + step) % 4
            send(yb.at[t, q, far], target, sent, sem, at(far, y, z, core))

        @pl.when(core != c)
        def _():
            send(yb.at[t, q, x], target, sent, sem, at(x, y, z, 1 - c))

        @pl.when(core == c)
        def _():
            pltpu.make_async_copy(yb.at[t, q, x], target, sem).start()

    def mine(t, stage):
        @pl.when(t % 2 == c)
        def _():
            stage(t // 2)

    def z_last(layer, q):
        done(gb.at[layer, 2 + q], x_sem.at[layer * 2 + q])

        @pl.when(q == 1)
        def _():
            target = gb.at[layer, jnp.where(outer, 2, 0)]
            send(gb.at[layer, 3], target, z_out.at[layer], z_sem.at[layer * 2], far_z)

        @pl.when((q == 0) & inner)
        def _():
            send(gb.at[layer, 2], gb.at[layer, 0], z_out.at[layer], z_sem.at[layer * 2 + 1], near_z)

    def z_last_relay(layer):
        @pl.when(outer)
        def _():
            done(gb.at[layer, 2], z_sem.at[layer * 2])
            send(gb.at[layer, 2], gb.at[layer, 1], z_out.at[layer], z_sem.at[layer * 2 + 1], near_z)

    def finish(layer, late):
        if late:
            done(gb.at[layer, 0], z_sem.at[layer * 2 + 1])

            @pl.when(inner)
            def _():
                done(gb.at[layer, 1], z_sem.at[layer * 2])

        else:
            done(gb.at[layer, 0], x_sem.at[layer * 2])
            done(gb.at[layer, 1], x_sem.at[layer * 2 + 1])
        gain = gv[pl.ds(layer, 1), :]
        for pair in range(PAIRS):
            arrived = gb[layer, 0:2, :, pair].reshape(256, FEATS)
            rows = jnp.dot(rm[pair // 2], arrived, preferred_element_type=jnp.float32) * gain
            ob[layer, pair * 256 : (pair + 1) * 256, :] = rows.astype(jnp.bfloat16)
        pltpu.make_async_copy(ob.at[layer], out_ref.at[layer], o_sem.at[layer]).start()

    sort_matrix(pm)
    for n in range(AHEAD):
        sort(n)
    load_gain.wait()
    load_rot.wait()
    pl.semaphore_wait(barrier, 23)
    for j in range(AHEAD // 2):
        z_first(LATE + j)
        along_y(j, 0)
        along_y(j, 1)

    def share_gain():
        @pl.when(ma // 2 == dev)
        def _():
            block = ma % 2
            pltpu.make_async_copy(gv, gs.at[block], gs_sem.at[block]).start()
            for step in range(1, 16):
                send(gv, gs.at[block], gs_out, gs_sem.at[block], {"dev": dev, "ma": (ma + step) % 16})

    def peaks(layer):
        @pl.when(layer == 0)
        def _():
            done(gs.at[0], gs_sem.at[0])
            done(gs.at[1], gs_sem.at[1])

        lane = lax.broadcasted_iota(jnp.int32, (192, 128), 1)
        for half in range(2):
            size = None
            for core in range(2):
                rows = sb[layer * 2 + core, place(layer * 2, half)].reshape(192, FEATS).astype(jnp.float32)
                rows = jnp.abs(rows * gs[core, pl.ds(layer, 1), :])
                rows = jnp.maximum(rows[:, :128], rows[:, 128:])
                size = rows if size is None else jnp.maximum(size, rows)
            top = jnp.max(size, axis=1, keepdims=True)
            part = slice(half * 192, (half + 1) * 192)
            pt[part, :] = jnp.where(lane == layer, top, pt[part, :])

        @pl.when(layer == LAYERS - 1)
        def _():
            for block in range(3):
                lanes = slice(block * 128, (block + 1) * 128)
                pk1[dev, :, lanes] = jnp.transpose(pt[lanes, :])[0:LAYERS, :].astype(jnp.bfloat16).astype(jnp.float32)

    def send_peaks():
        for step in range(1, 8):
            send(pk1.at[dev], pk1.at[dev], pk1_out, pk1_sem, {"dev": (dev + step) % 8, "ma": ma})

    def group_peaks():
        done(pk1.at[0:7], pk1_sem)
        top = jnp.max(pk1[...], axis=0).astype(jnp.bfloat16)
        row = lax.broadcasted_iota(jnp.int32, (COLS, 128), 0)
        lane = lax.broadcasted_iota(jnp.int32, (COLS, 128), 1)
        pick = jnp.where((row - dev * PIECE == lane) & (lane < PIECE), 1.0, 0.0).astype(jnp.bfloat16)
        pk2[ma] = jnp.dot(top, pick, preferred_element_type=jnp.float32)

    def spread_peaks():
        for step in range(1, 16):
            send(pk2.at[ma], pk2.at[ma], pk2_out, pk2_sem, {"dev": dev, "ma": (ma + step) % 16})

    def last_peaks():
        done(pk2.at[0:15], pk2_sem)
        lane = lax.broadcasted_iota(jnp.int32, (LAYERS, 128), 1)
        for pair in range(PAIRS):
            halves = []
            for half in range(2):
                line = jnp.zeros((LAYERS, 128), jnp.float32)
                for piece in range(8):
                    shift = (piece - pair) * 16 % 128
                    part = pk2[half * 8 + piece]
                    part = pltpu.roll(part, shift, 1) if shift else part
                    line = jnp.where((lane >= piece * 16) & (lane < piece * 16 + 16), part, line)
                halves.append(line)
            low = jnp.where(zl == 1, halves[0], halves[1])
            high = jnp.where(zl == 1, halves[1], halves[0])
            line = jnp.concatenate([low, high], axis=1).astype(jnp.bfloat16)
            peak_ref[:, pair * 256 : (pair + 1) * 256] = lax.dot_general(
                line, rm[pair // 2], (((1,), (1,)), ((), ())), preferred_element_type=jnp.float32
            )

    def turn(i, carry):
        def halves(at_step, stage, first, last):
            v = i - at_step

            @pl.when((v >= first) & (v < last))
            def _():
                stage(v // 2, v % 2)

        def chunks(at_step, stage, first, last):
            v = i - at_step

            @pl.when((v >= 2 * first) & (v < 2 * last) & (v % 2 == 0))
            def _():
                stage(v // 2)

        halves(0, along_x, 0, STEPS)
        halves(1 - AHEAD, along_y, AHEAD, STEPS)
        chunks(2 - AHEAD, lambda j: z_first(LATE + j), AHEAD // 2, CHUNKS - LATE)
        chunks(Z_FIRST_RELAY, lambda j: z_first_relay(LATE + j), 0, CHUNKS - LATE)
        halves(Z_LAST, lambda t, q: mine(t, lambda layer: z_last(layer, q)), 0, 2 * LATE)
        chunks(Z_LAST_RELAY, lambda t: mine(t, z_last_relay), 0, LATE)

        @pl.when(i < CHUNKS - AHEAD)
        def _():
            sort(i + AHEAD)

        chunks(FINISH_LATE, lambda t: mine(t, lambda layer: finish(layer, True)), 0, LATE)
        chunks(FINISH, lambda j: mine(LATE + j, lambda layer: finish(layer, False)), 0, CHUNKS - LATE)

        @pl.when((i >= PEAKS_FROM) & (i < PEAKS_FROM + 2 * LAYERS) & (i % 2 == 0))
        def _():
            peaks((i - PEAKS_FROM) // 2)

        pl.when(i == PEAKS_SEND)(send_peaks)
        pl.when(i == PEAKS_GROUP)(group_peaks)
        pl.when(i == PEAKS_SPREAD)(spread_peaks)
        pl.when(i == PEAKS_LAST)(last_peaks)

        @pl.when(i == 0)
        def _():
            share_gain()
            order_matrix(rv, rm, zl)

        return carry

    lax.fori_loop(0, END, turn, 0)

    def close(t, carry):
        done(sb.at[t, 0:2, 0:3], y_out.at[t])

        @pl.when(t >= LATE)
        def _():
            done(sb.at[t, 2:4], first_out.at[t])

        @pl.when(t % 2 == c)
        def _():
            done(yb.at[t, :, 0:3], x_out.at[t])

        @pl.when(t % 2 != c)
        def _():
            done(yb.at[t], x_out.at[t])

        return carry

    lax.fori_loop(0, CHUNKS, close, 0)

    def close_layer(layer, carry):
        @pl.when(layer < LATE // 2)
        def _():
            done(gb.at[layer, 2:4], z_out.at[layer])

        done(ob.at[layer], o_sem.at[layer])
        return carry

    lax.fori_loop(0, LAYERS, close_layer, 0)

    @pl.when(ma // 2 == dev)
    def _():
        done(gs.at[0:15], gs_out)

    done(pk1.at[0:7], pk1_out)
    done(pk2.at[0:15], pk2_out)


def write_out(tiles_ref, peak_ref, q_ref, k_ref, v_ref, row_ref, sem):
    copies = [
        pltpu.make_async_copy(tiles_ref.at[:, pl.ds(0, 512)], q_ref, sem.at[0]),
        pltpu.make_async_copy(tiles_ref.at[:, pl.ds(512, 128)], k_ref, sem.at[1]),
        pltpu.make_async_copy(tiles_ref.at[:, pl.ds(640, 128)], v_ref, sem.at[2]),
        pltpu.make_async_copy(peak_ref, row_ref, sem.at[3]),
    ]
    for copy in copies:
        copy.start()
    for copy in copies:
        copy.wait()


def shards(joined_weight, norm_gain, rotary_order):
    dma = pltpu.SemaphoreType.DMA
    bf16, f32 = jnp.bfloat16, jnp.float32
    hbm = pl.BlockSpec(memory_space=pltpu.HBM)
    anywhere = pl.BlockSpec(memory_space=pl.ANY)
    tiles, peak = pl.pallas_call(
        kernel,
        name="relayout",
        out_shape=(jax.ShapeDtypeStruct((LAYERS, 768, FEATS), bf16), jax.ShapeDtypeStruct((LAYERS, 768), f32)),
        in_specs=[hbm, hbm, hbm],
        out_specs=(anywhere, pl.BlockSpec(memory_space=pltpu.VMEM)),
        scratch_shapes=[
            pltpu.VMEM((1, 128), jnp.int32),
            pltpu.VMEM((LAYERS, FEATS), f32),
            pltpu.VMEM((15, LAYERS, FEATS), f32),
            pltpu.VMEM((CHUNKS, FEATS, COLS), bf16),
            pltpu.VMEM((CHUNKS, 4, 4, PAIRS, 16, FEATS), bf16),
            pltpu.VMEM((CHUNKS, 2, 4, PAIRS, 16, FEATS), bf16),
            pltpu.VMEM((LAYERS, 4, 8, PAIRS, 16, FEATS), bf16),
            pltpu.VMEM((LAYERS, 768, FEATS), bf16),
            pltpu.VMEM((COLS, 128), f32),
            pltpu.VMEM((8, LAYERS, COLS), f32),
            pltpu.VMEM((16, LAYERS, 128), f32),
            pltpu.VMEM((COLS, COLS), bf16),
            pltpu.VMEM((2, 256, 256), bf16),
            dma((CHUNKS,)),
            dma,
            dma,
            dma((2,)),
            dma,
            dma((CHUNKS,)),
            dma((CHUNKS,)),
            dma((CHUNKS * 2,)),
            dma((LAYERS * 2,)),
            dma((LAYERS * 2,)),
            dma((CHUNKS,)),
            dma((CHUNKS,)),
            dma((CHUNKS,)),
            dma((LAYERS,)),
            dma((LAYERS,)),
            dma,
            dma,
            dma,
            dma,
        ],
        compiler_params=pltpu.CompilerParams(collective_id=0, has_side_effects=True, vmem_limit_bytes=40 * 2**20),
    )(*(pltpu.with_memory_space_constraint(a, pltpu.HBM) for a in (rotary_order.reshape(1, 128), norm_gain, joined_weight)))
    return pl.pallas_call(
        write_out,
        name="write_out",
        out_shape=(
            jax.ShapeDtypeStruct((LAYERS, 512, FEATS), bf16),
            jax.ShapeDtypeStruct((LAYERS, 128, FEATS), bf16),
            jax.ShapeDtypeStruct((LAYERS, 128, FEATS), bf16),
            jax.ShapeDtypeStruct((LAYERS, 768), f32),
        ),
        in_specs=[anywhere, anywhere],
        out_specs=(hbm, hbm, hbm, hbm),
        scratch_shapes=[dma((4,))],
        compiler_params=pltpu.CompilerParams(vmem_limit_bytes=2**20),
    )(tiles, peak)


def solution(mesh):
    placed = (P(None, "dev", "ma"), P(None, "ma"), P())
    tiles = P(None, "dev", "ma")
    return jax.shard_map(shards, mesh=mesh, in_specs=placed, out_specs=(tiles, tiles, tiles, P(None, "dev")), check_vma=False)
```

```python
import jax
import jax.numpy as jnp
from jax import lax
from jax.experimental import pallas as pl
from jax.experimental.pallas import tpu as pltpu
from jax.sharding import PartitionSpec as P

LAYERS = 8
CHUNKS = 16
FEATS = 256
COLS = 384
PIECE = 48
PAIRS = 3
LATE = 8
AHEAD = 8
LEAD = 7
SHARE, MATRIX = 0, 2
STEPS = 2 * CHUNKS
Z_LAST, Z_LAST_RELAY, Z_FIRST_RELAY, FINISH_LATE, FINISH = 7, 18, 3, 23, 21
PEAKS_FROM, PEAKS_SEND, PEAKS_GROUP, PEAKS_SPREAD, PEAKS_LAST = 6, 14, 24, 25, 34
END = max(FINISH, FINISH_LATE) + 15
MESH = pl.DeviceIdType.MESH


def sort_matrix(pm_ref):
    row = lax.broadcasted_iota(jnp.int32, (COLS, 128), 0)
    lane = lax.broadcasted_iota(jnp.int32, (COLS, 128), 1)
    g = (row * 1366) >> 16
    rest = row - g * PIECE
    s, dd = rest >> 3, rest & 7
    head = jnp.where(s < 4, g * 4 + s, 32 + (s - 4) * 8 + g)
    column = dd * PIECE + head
    for block in range(COLS // 128):
        pm_ref[:, block * 128 : (block + 1) * 128] = jnp.where(column == lane + block * 128, 1.0, 0.0).astype(jnp.bfloat16)


def order_matrix(rot_ref, rm_ref, zl):
    turned = jnp.transpose(jnp.broadcast_to(rot_ref[0:1, :], (128, 128)))
    plain = lax.broadcasted_iota(jnp.int32, (128, 128), 0)
    lane = lax.broadcasted_iota(jnp.int32, (128, 128), 1)

    def hot(stored, s2, block):
        piece = stored >> 3
        half = piece >> 3
        slot = jnp.where(zl == 1, half, 1 - half)
        column = slot * 128 + (piece & 7) * 16 + s2 * 8 + (stored & 7)
        return jnp.where(column == lane + block * 128, 1.0, 0.0).astype(jnp.bfloat16)

    for block in range(2):
        lanes = slice(block * 128, (block + 1) * 128)
        key = hot(turned, 0, block)
        rm_ref[0, 0:128, lanes] = key
        rm_ref[1, 0:128, lanes] = key
        rm_ref[0, 128:256, lanes] = hot(turned, 1, block)
        rm_ref[1, 128:256, lanes] = hot(plain, 1, block)


def kernel(
    rot_ref, gain_ref, w_ref, out_ref, peak_ref,
    rv, gv, gs, xb, sb, yb, gb, ob, pt, pk1, pk2, pm, rm,
    in_sem, rot_sem, gain_sem, gs_sem, gs_out, far_sem, near_sem, y_sem, x_sem, z_sem, first_out, y_out, x_out, z_out, o_sem,
    pk1_sem, pk1_out, pk2_sem, pk2_out,
):
    dev, ma = lax.axis_index("dev"), lax.axis_index("ma")
    zh, y = dev // 4, dev % 4
    zl, x, c = ma // 8, (ma // 2) % 4, ma % 2
    z = zh * 2 + zl
    inner = (z == 1) | (z == 2)
    outer = (z == 0) | (z == 3)
    far_z = {"dev": (1 - zh) * 4 + y, "ma": (1 - zl) * 8 + x * 2 + c}
    near_z = {"dev": dev, "ma": (1 - zl) * 8 + x * 2 + c}

    def at(x_, y_, z_, c_):
        return {"dev": (z_ // 2) * 4 + y_, "ma": (z_ % 2) * 8 + x_ * 2 + c_}

    def send(src, dst, out_sem, in_sem_, device):
        pltpu.make_async_remote_copy(src, dst, out_sem, in_sem_, device_id=device, device_id_type=MESH).start()

    def done(ref, sem):
        pltpu.make_async_copy(ref, ref, sem).wait()

    def load(t):
        return pltpu.make_async_copy(w_ref.at[t // 2, pl.ds((t % 2) * FEATS, FEATS), :], xb.at[t], in_sem.at[t])

    load_rot = pltpu.make_async_copy(rot_ref, rv, rot_sem)
    load_gain = pltpu.make_async_copy(gain_ref, gv, gain_sem)

    for n in range(CHUNKS):
        load(n // 2 + (n % 2) * LATE).start()
    load_rot.start()
    load_gain.start()

    barrier = pltpu.get_barrier_semaphore()
    for step in range(1, 16):
        pl.semaphore_signal(barrier, inc=1, device_id={"dev": dev, "ma": (ma + step) % 16}, device_id_type=MESH)
    for step in range(1, 8):
        pl.semaphore_signal(barrier, inc=1, device_id={"dev": (dev + step) % 8, "ma": ma}, device_id_type=MESH)
    pl.semaphore_signal(barrier, inc=1, device_id=far_z, device_id_type=MESH)

    def place(t, half):
        kept = zh == half
        early = jnp.where(kept, jnp.where(outer, 0, 3), 2)
        return jnp.where(t < LATE, jnp.where(kept, 0, 1), early)

    def sort(n):
        t = n // 2 + (n % 2) * LATE
        load(t).wait()
        rows = lax.dot_general(pm[...], xb[t], (((1,), (1,)), ((), ())), preferred_element_type=jnp.float32)
        rows = rows.astype(jnp.bfloat16).reshape(2, 4, PAIRS, 16, FEATS)
        sb[t, place(t, 0)] = rows[0]
        sb[t, place(t, 1)] = rows[1]

    def z_first(t):
        send(sb.at[t, 2], sb.at[t, jnp.where(outer, 3, 0)], first_out.at[t], far_sem.at[t], far_z)

        @pl.when(inner)
        def _():
            send(sb.at[t, 3], sb.at[t, 1], first_out.at[t], near_sem.at[t], near_z)

    def z_first_relay(t):
        @pl.when(outer)
        def _():
            done(sb.at[t, 3], far_sem.at[t])
            send(sb.at[t, 3], sb.at[t, 1], first_out.at[t], near_sem.at[t], near_z)

    def along_y(t, q):
        @pl.when((t >= LATE) & (q == 0) & inner)
        def _():
            done(sb.at[t, 0], far_sem.at[t])

        @pl.when((t >= LATE) & (q == 1))
        def _():
            done(sb.at[t, 1], near_sem.at[t])

        pltpu.make_async_copy(sb.at[t, q, y], yb.at[t, q, y], y_sem.at[t * 2 + q]).start()
        for step in (2, 1, 3):
            far = (y + step) % 4
            send(sb.at[t, q, far], yb.at[t, q, y], y_out.at[t], y_sem.at[t * 2 + q], at(x, far, z, c))

    def along_x(t, q):
        layer, core = t // 2, t % 2
        sent, sem = x_out.at[t], x_sem.at[layer * 2 + q]
        done(yb.at[t, q], y_sem.at[t * 2 + q])
        late = jnp.where(q == 1, 3, jnp.where(outer, 1, 2))
        slot = jnp.where(t < LATE, late, jnp.where(outer, 1 - q, q))
        target = gb.at[layer, slot, x * 2 + c]
        for step in (2, 1, 3):
            far = (x + step) % 4
            send(yb.at[t, q, far], target, sent, sem, at(far, y, z, core))

        @pl.when(core != c)
        def _():
            send(yb.at[t, q, x], target, sent, sem, at(x, y, z, 1 - c))

        @pl.when(core == c)
        def _():
            pltpu.make_async_copy(yb.at[t, q, x], target, sem).start()

    def mine(t, stage):
        @pl.when(t % 2 == c)
        def _():
            stage(t // 2)

    def z_last(layer, q):
        done(gb.at[layer, 2 + q], x_sem.at[layer * 2 + q])

        @pl.when(q == 1)
        def _():
            target = gb.at[layer, jnp.where(outer, 2, 0)]
            send(gb.at[layer, 3], target, z_out.at[layer], z_sem.at[layer * 2], far_z)

        @pl.when((q == 0) & inner)
        def _():
            send(gb.at[layer, 2], gb.at[layer, 0], z_out.at[layer], z_sem.at[layer * 2 + 1], near_z)

    def z_last_relay(layer):
        @pl.when(outer)
        def _():
            done(gb.at[layer, 2], z_sem.at[layer * 2])
            send(gb.at[layer, 2], gb.at[layer, 1], z_out.at[layer], z_sem.at[layer * 2 + 1], near_z)

    def finish(layer, late):
        if late:
            done(gb.at[layer, 0], z_sem.at[layer * 2 + 1])

            @pl.when(inner)
            def _():
                done(gb.at[layer, 1], z_sem.at[layer * 2])

        else:
            done(gb.at[layer, 0], x_sem.at[layer * 2])
            done(gb.at[layer, 1], x_sem.at[layer * 2 + 1])
        gain = gv[pl.ds(layer, 1), :]
        for pair in range(PAIRS):
            arrived = gb[layer, 0:2, :, pair].reshape(256, FEATS)
            rows = jnp.dot(rm[pair // 2], arrived, preferred_element_type=jnp.float32) * gain
            ob[layer, pair * 256 : (pair + 1) * 256, :] = rows.astype(jnp.bfloat16)
        pltpu.make_async_copy(ob.at[layer], out_ref.at[layer], o_sem.at[layer]).start()

    def first_send(n):
        @pl.when(n % 2 == 0)
        def _():
            along_y(n // 2, 0)
            along_y(n // 2, 1)

        @pl.when(n % 2 == 1)
        def _():
            z_first(LATE + n // 2)

    def start(n, carry):
        sort(n)
        first_send(n - 1)
        return carry

    sort_matrix(pm)
    sort(0)
    load_gain.wait()
    load_rot.wait()
    pl.semaphore_wait(barrier, 23)
    lax.fori_loop(1, AHEAD, start, 0)

    def share_gain():
        @pl.when(ma // 2 == dev)
        def _():
            block = ma % 2
            pltpu.make_async_copy(gv, gs.at[block], gs_sem.at[block]).start()
            for step in range(1, 16):
                send(gv, gs.at[block], gs_out, gs_sem.at[block], {"dev": dev, "ma": (ma + step) % 16})

    def peaks(layer):
        @pl.when(layer == 0)
        def _():
            done(gs.at[0], gs_sem.at[0])
            done(gs.at[1], gs_sem.at[1])

        lane = lax.broadcasted_iota(jnp.int32, (192, 128), 1)
        for half in range(2):
            size = None
            for core in range(2):
                rows = sb[layer * 2 + core, place(layer * 2, half)].reshape(192, FEATS).astype(jnp.float32)
                rows = jnp.abs(rows * gs[core, pl.ds(layer, 1), :])
                rows = jnp.maximum(rows[:, :128], rows[:, 128:])
                size = rows if size is None else jnp.maximum(size, rows)
            top = jnp.max(size, axis=1, keepdims=True)
            part = slice(half * 192, (half + 1) * 192)
            pt[part, :] = jnp.where(lane == layer, top, pt[part, :])

        @pl.when(layer == LAYERS - 1)
        def _():
            for block in range(3):
                lanes = slice(block * 128, (block + 1) * 128)
                pk1[dev, :, lanes] = jnp.transpose(pt[lanes, :])[0:LAYERS, :].astype(jnp.bfloat16).astype(jnp.float32)

    def send_peaks():
        for step in range(1, 8):
            send(pk1.at[dev], pk1.at[dev], pk1_out, pk1_sem, {"dev": (dev + step) % 8, "ma": ma})

    def group_peaks():
        done(pk1.at[0:7], pk1_sem)
        top = jnp.max(pk1[...], axis=0).astype(jnp.bfloat16)
        row = lax.broadcasted_iota(jnp.int32, (COLS, 128), 0)
        lane = lax.broadcasted_iota(jnp.int32, (COLS, 128), 1)
        pick = jnp.where((row - dev * PIECE == lane) & (lane < PIECE), 1.0, 0.0).astype(jnp.bfloat16)
        pk2[ma] = jnp.dot(top, pick, preferred_element_type=jnp.float32)

    def spread_peaks():
        for step in range(1, 16):
            send(pk2.at[ma], pk2.at[ma], pk2_out, pk2_sem, {"dev": dev, "ma": (ma + step) % 16})

    def last_peaks():
        done(pk2.at[0:15], pk2_sem)
        lane = lax.broadcasted_iota(jnp.int32, (LAYERS, 128), 1)
        for pair in range(PAIRS):
            halves = []
            for half in range(2):
                line = jnp.zeros((LAYERS, 128), jnp.float32)
                for piece in range(8):
                    shift = (piece - pair) * 16 % 128
                    part = pk2[half * 8 + piece]
                    part = pltpu.roll(part, shift, 1) if shift else part
                    line = jnp.where((lane >= piece * 16) & (lane < piece * 16 + 16), part, line)
                halves.append(line)
            low = jnp.where(zl == 1, halves[0], halves[1])
            high = jnp.where(zl == 1, halves[1], halves[0])
            line = jnp.concatenate([low, high], axis=1).astype(jnp.bfloat16)
            peak_ref[:, pair * 256 : (pair + 1) * 256] = lax.dot_general(
                line, rm[pair // 2], (((1,), (1,)), ((), ())), preferred_element_type=jnp.float32
            )

    def turn(i, carry):
        def halves(at_step, stage, first, last):
            v = i - at_step

            @pl.when((v >= first) & (v < last))
            def _():
                stage(v // 2, v % 2)

        def chunks(at_step, stage, first, last):
            v = i - at_step

            @pl.when((v >= 2 * first) & (v < 2 * last) & (v % 2 == 0))
            def _():
                stage(v // 2)

        halves(0, along_x, 0, STEPS)
        pl.when(i <= CHUNKS - AHEAD)(lambda: first_send(i + AHEAD - 1))
        halves(-LEAD, along_y, 2 * LATE, STEPS)
        chunks(Z_FIRST_RELAY, lambda j: z_first_relay(LATE + j), 0, CHUNKS - LATE)
        halves(Z_LAST, lambda t, q: mine(t, lambda layer: z_last(layer, q)), 0, 2 * LATE)
        chunks(Z_LAST_RELAY, lambda t: mine(t, z_last_relay), 0, LATE)

        @pl.when(i < CHUNKS - AHEAD)
        def _():
            sort(i + AHEAD)

        chunks(FINISH_LATE, lambda t: mine(t, lambda layer: finish(layer, True)), 0, LATE)
        chunks(FINISH, lambda j: mine(LATE + j, lambda layer: finish(layer, False)), 0, CHUNKS - LATE)

        @pl.when((i >= PEAKS_FROM) & (i < PEAKS_FROM + LAYERS))
        def _():
            peaks(i - PEAKS_FROM)

        pl.when(i == PEAKS_SEND)(send_peaks)
        pl.when(i == PEAKS_GROUP)(group_peaks)
        pl.when(i == PEAKS_SPREAD)(spread_peaks)
        pl.when(i == PEAKS_LAST)(last_peaks)

        pl.when(i == SHARE)(share_gain)
        pl.when(i == MATRIX)(lambda: order_matrix(rv, rm, zl))

        return carry

    lax.fori_loop(0, END, turn, 0)

    def close(t, carry):
        done(sb.at[t, 0:2, 0:3], y_out.at[t])

        @pl.when(t >= LATE)
        def _():
            done(sb.at[t, 2:4], first_out.at[t])

        @pl.when(t % 2 == c)
        def _():
            done(yb.at[t, :, 0:3], x_out.at[t])

        @pl.when(t % 2 != c)
        def _():
            done(yb.at[t], x_out.at[t])

        return carry

    lax.fori_loop(0, CHUNKS, close, 0)

    def close_layer(layer, carry):
        @pl.when(layer < LATE // 2)
        def _():
            done(gb.at[layer, 2:4], z_out.at[layer])

        done(ob.at[layer], o_sem.at[layer])
        return carry

    lax.fori_loop(0, LAYERS, close_layer, 0)

    @pl.when(ma // 2 == dev)
    def _():
        done(gs.at[0:15], gs_out)

    done(pk1.at[0:7], pk1_out)
    done(pk2.at[0:15], pk2_out)


def write_out(tiles_ref, peak_ref, q_ref, k_ref, v_ref, row_ref, sem):
    copies = [
        pltpu.make_async_copy(tiles_ref.at[:, pl.ds(0, 512)], q_ref, sem.at[0]),
        pltpu.make_async_copy(tiles_ref.at[:, pl.ds(512, 128)], k_ref, sem.at[1]),
        pltpu.make_async_copy(tiles_ref.at[:, pl.ds(640, 128)], v_ref, sem.at[2]),
        pltpu.make_async_copy(peak_ref, row_ref, sem.at[3]),
    ]
    for copy in copies:
        copy.start()
    for copy in copies:
        copy.wait()


def shards(joined_weight, norm_gain, rotary_order):
    dma = pltpu.SemaphoreType.DMA
    bf16, f32 = jnp.bfloat16, jnp.float32
    hbm = pl.BlockSpec(memory_space=pltpu.HBM)
    anywhere = pl.BlockSpec(memory_space=pl.ANY)
    tiles, peak = pl.pallas_call(
        kernel,
        name="relayout",
        out_shape=(jax.ShapeDtypeStruct((LAYERS, 768, FEATS), bf16), jax.ShapeDtypeStruct((LAYERS, 768), f32)),
        in_specs=[hbm, hbm, hbm],
        out_specs=(anywhere, pl.BlockSpec(memory_space=pltpu.VMEM)),
        scratch_shapes=[
            pltpu.VMEM((1, 128), jnp.int32),
            pltpu.VMEM((LAYERS, FEATS), f32),
            pltpu.VMEM((15, LAYERS, FEATS), f32),
            pltpu.VMEM((CHUNKS, FEATS, COLS), bf16),
            pltpu.VMEM((CHUNKS, 4, 4, PAIRS, 16, FEATS), bf16),
            pltpu.VMEM((CHUNKS, 2, 4, PAIRS, 16, FEATS), bf16),
            pltpu.VMEM((LAYERS, 4, 8, PAIRS, 16, FEATS), bf16),
            pltpu.VMEM((LAYERS, 768, FEATS), bf16),
            pltpu.VMEM((COLS, 128), f32),
            pltpu.VMEM((8, LAYERS, COLS), f32),
            pltpu.VMEM((16, LAYERS, 128), f32),
            pltpu.VMEM((COLS, COLS), bf16),
            pltpu.VMEM((2, 256, 256), bf16),
            dma((CHUNKS,)),
            dma,
            dma,
            dma((2,)),
            dma,
            dma((CHUNKS,)),
            dma((CHUNKS,)),
            dma((CHUNKS * 2,)),
            dma((LAYERS * 2,)),
            dma((LAYERS * 2,)),
            dma((CHUNKS,)),
            dma((CHUNKS,)),
            dma((CHUNKS,)),
            dma((LAYERS,)),
            dma((LAYERS,)),
            dma,
            dma,
            dma,
            dma,
        ],
        compiler_params=pltpu.CompilerParams(collective_id=0, has_side_effects=True, vmem_limit_bytes=40 * 2**20),
    )(*(pltpu.with_memory_space_constraint(a, pltpu.HBM) for a in (rotary_order.reshape(1, 128), norm_gain, joined_weight)))
    return pl.pallas_call(
        write_out,
        name="write_out",
        out_shape=(
            jax.ShapeDtypeStruct((LAYERS, 512, FEATS), bf16),
            jax.ShapeDtypeStruct((LAYERS, 128, FEATS), bf16),
            jax.ShapeDtypeStruct((LAYERS, 128, FEATS), bf16),
            jax.ShapeDtypeStruct((LAYERS, 768), f32),
        ),
        in_specs=[anywhere, anywhere],
        out_specs=(hbm, hbm, hbm, hbm),
        scratch_shapes=[dma((4,))],
        compiler_params=pltpu.CompilerParams(vmem_limit_bytes=2**20),
    )(tiles, peak)


def solution(mesh):
    placed = (P(None, "dev", "ma"), P(None, "ma"), P())
    tiles = P(None, "dev", "ma")
    return jax.shard_map(shards, mesh=mesh, in_specs=placed, out_specs=(tiles, tiles, tiles, P(None, "dev")), check_vma=False)
```

```python
import jax
import jax.numpy as jnp
from jax import lax
from jax.experimental import pallas as pl
from jax.experimental.pallas import tpu as pltpu
from jax.sharding import PartitionSpec as P

LAYERS = 8
CHUNKS = 16
FEATS = 256
COLS = 384
PIECE = 48
PAIRS = 3
LATE = 8
AHEAD = 8
LEAD = 5
SHARE, MATRIX, CLOSE = 0, 2, 5
STEPS = 2 * CHUNKS
Z_LAST, Z_LAST_RELAY, Z_FIRST_RELAY, FINISH_LATE, FINISH = 7, 18, 3, 23, 21
PEAKS_FROM, PEAKS_SEND, PEAKS_GROUP, PEAKS_SPREAD, PEAKS_LAST = 6, 15, 29, 30, 37
END = max(FINISH, FINISH_LATE) + 15
MESH = pl.DeviceIdType.MESH


def sort_matrix(pm_ref):
    row = lax.broadcasted_iota(jnp.int32, (COLS, 128), 0)
    lane = lax.broadcasted_iota(jnp.int32, (COLS, 128), 1)
    g = (row * 1366) >> 16
    rest = row - g * PIECE
    s, dd = rest >> 3, rest & 7
    head = jnp.where(s < 4, g * 4 + s, 32 + (s - 4) * 8 + g)
    column = dd * PIECE + head
    for block in range(COLS // 128):
        pm_ref[:, block * 128 : (block + 1) * 128] = jnp.where(column == lane + block * 128, 1.0, 0.0).astype(jnp.bfloat16)


def order_matrix(rot_ref, rm_ref, zl):
    turned = jnp.transpose(jnp.broadcast_to(rot_ref[0:1, :], (128, 128)))
    plain = lax.broadcasted_iota(jnp.int32, (128, 128), 0)
    lane = lax.broadcasted_iota(jnp.int32, (128, 128), 1)

    def hot(stored, s2, block):
        piece = stored >> 3
        half = piece >> 3
        slot = jnp.where(zl == 1, half, 1 - half)
        column = slot * 128 + (piece & 7) * 16 + s2 * 8 + (stored & 7)
        return jnp.where(column == lane + block * 128, 1.0, 0.0).astype(jnp.bfloat16)

    for block in range(2):
        lanes = slice(block * 128, (block + 1) * 128)
        key = hot(turned, 0, block)
        rm_ref[0, 0:128, lanes] = key
        rm_ref[1, 0:128, lanes] = key
        rm_ref[0, 128:256, lanes] = hot(turned, 1, block)
        rm_ref[1, 128:256, lanes] = hot(plain, 1, block)


def kernel(
    rot_ref, gain_ref, w_ref, out_ref, peak_ref,
    rv, gv, gs, xb, sb, yb, gb, pt, pt2, pk0, pk1, pk2, pm, rm,
    in_sem, rot_sem, gain_sem, gs_sem, gs_out, far_sem, near_sem, y_sem, x_sem, z_sem, first_out, y_out, x_out, z_out,
    pk1_sem, pk1_out, pk2_sem, pk2_out,
):
    dev, ma = lax.axis_index("dev"), lax.axis_index("ma")
    zh, y = dev // 4, dev % 4
    zl, x, c = ma // 8, (ma // 2) % 4, ma % 2
    z = zh * 2 + zl
    inner = (z == 1) | (z == 2)
    outer = (z == 0) | (z == 3)
    far_z = {"dev": (1 - zh) * 4 + y, "ma": (1 - zl) * 8 + x * 2 + c}
    near_z = {"dev": dev, "ma": (1 - zl) * 8 + x * 2 + c}

    def at(x_, y_, z_, c_):
        return {"dev": (z_ // 2) * 4 + y_, "ma": (z_ % 2) * 8 + x_ * 2 + c_}

    def send(src, dst, out_sem, in_sem_, device):
        pltpu.make_async_remote_copy(src, dst, out_sem, in_sem_, device_id=device, device_id_type=MESH).start()

    def done(ref, sem):
        pltpu.make_async_copy(ref, ref, sem).wait()

    def load(t):
        return pltpu.make_async_copy(w_ref.at[t // 2, pl.ds((t % 2) * FEATS, FEATS), :], xb.at[t], in_sem.at[t])

    load_rot = pltpu.make_async_copy(rot_ref, rv, rot_sem)
    load_gain = pltpu.make_async_copy(gain_ref, gv, gain_sem)

    for n in range(CHUNKS):
        load(n // 2 + (n % 2) * LATE).start()
    load_rot.start()
    load_gain.start()

    barrier = pltpu.get_barrier_semaphore()
    for step in range(1, 16):
        pl.semaphore_signal(barrier, inc=1, device_id={"dev": dev, "ma": (ma + step) % 16}, device_id_type=MESH)
    for step in range(1, 8):
        pl.semaphore_signal(barrier, inc=1, device_id={"dev": (dev + step) % 8, "ma": ma}, device_id_type=MESH)
    pl.semaphore_signal(barrier, inc=1, device_id=far_z, device_id_type=MESH)

    def place(t, half):
        kept = zh == half
        early = jnp.where(kept, jnp.where(outer, 0, 3), 2)
        return jnp.where(t < LATE, jnp.where(kept, 0, 1), early)

    def sort(n):
        t = n // 2 + (n % 2) * LATE
        load(t).wait()
        rows = lax.dot_general(pm[...], xb[t], (((1,), (1,)), ((), ())), preferred_element_type=jnp.float32)
        rows = rows.astype(jnp.bfloat16).reshape(2, 4, PAIRS, 16, FEATS)
        sb[t, place(t, 0)] = rows[0]
        sb[t, place(t, 1)] = rows[1]

    def z_first(t):
        send(sb.at[t, 2], sb.at[t, jnp.where(outer, 3, 0)], first_out.at[t], far_sem.at[t], far_z)

        @pl.when(inner)
        def _():
            send(sb.at[t, 3], sb.at[t, 1], first_out.at[t], near_sem.at[t], near_z)

    def z_first_relay(t):
        @pl.when(outer)
        def _():
            done(sb.at[t, 3], far_sem.at[t])
            send(sb.at[t, 3], sb.at[t, 1], first_out.at[t], near_sem.at[t], near_z)

    def along_y(t, q):
        @pl.when((t >= LATE) & (q == 0) & inner)
        def _():
            done(sb.at[t, 0], far_sem.at[t])

        @pl.when((t >= LATE) & (q == 1))
        def _():
            done(sb.at[t, 1], near_sem.at[t])

        pltpu.make_async_copy(sb.at[t, q, y], yb.at[t, q, y], y_sem.at[t * 2 + q]).start()
        for step in (2, 1, 3):
            far = (y + step) % 4
            send(sb.at[t, q, far], yb.at[t, q, y], y_out.at[t], y_sem.at[t * 2 + q], at(x, far, z, c))

    def along_x(t, q):
        layer, core = t // 2, t % 2
        sent, sem = x_out.at[t], x_sem.at[layer * 2 + q]
        done(yb.at[t, q], y_sem.at[t * 2 + q])
        late = jnp.where(q == 1, 3, jnp.where(outer, 1, 2))
        slot = jnp.where(t < LATE, late, jnp.where(outer, 1 - q, q))
        target = gb.at[layer, slot, x * 2 + c]
        for step in (2, 1, 3):
            far = (x + step) % 4
            send(yb.at[t, q, far], target, sent, sem, at(far, y, z, core))

        @pl.when(core != c)
        def _():
            send(yb.at[t, q, x], target, sent, sem, at(x, y, z, 1 - c))

        @pl.when(core == c)
        def _():
            pltpu.make_async_copy(yb.at[t, q, x], target, sem).start()

    def mine(t, stage):
        @pl.when(t % 2 == c)
        def _():
            stage(t // 2)

    def z_last(layer, q):
        done(gb.at[layer, 2 + q], x_sem.at[layer * 2 + q])

        @pl.when(q == 1)
        def _():
            target = gb.at[layer, jnp.where(outer, 2, 0)]
            send(gb.at[layer, 3], target, z_out.at[layer], z_sem.at[layer * 2], far_z)

        @pl.when((q == 0) & inner)
        def _():
            send(gb.at[layer, 2], gb.at[layer, 0], z_out.at[layer], z_sem.at[layer * 2 + 1], near_z)

    def z_last_relay(layer):
        @pl.when(outer)
        def _():
            done(gb.at[layer, 2], z_sem.at[layer * 2])
            send(gb.at[layer, 2], gb.at[layer, 1], z_out.at[layer], z_sem.at[layer * 2 + 1], near_z)

    def finish(layer, late):
        if late:
            done(gb.at[layer, 0], z_sem.at[layer * 2 + 1])

            @pl.when(inner)
            def _():
                done(gb.at[layer, 1], z_sem.at[layer * 2])

        else:
            done(gb.at[layer, 0], x_sem.at[layer * 2])
            done(gb.at[layer, 1], x_sem.at[layer * 2 + 1])
        gain = gv[pl.ds(layer, 1), :]
        for pair in range(PAIRS):
            arrived = gb[layer, 0:2, :, pair].reshape(256, FEATS)
            rows = jnp.dot(rm[pair // 2], arrived, preferred_element_type=jnp.float32) * gain
            out_ref[layer, pair * 256 : (pair + 1) * 256, :] = rows.astype(jnp.bfloat16)

    def first_send(n):
        @pl.when(n % 2 == 0)
        def _():
            along_y(n // 2, 0)
            along_y(n // 2, 1)

        @pl.when(n % 2 == 1)
        def _():
            z_first(LATE + n // 2)

    def start(n, carry):
        sort(n)
        first_send(n - 1)
        return carry

    sort_matrix(pm)
    sort(0)
    load_gain.wait()
    load_rot.wait()
    pl.semaphore_wait(barrier, 23)
    lax.fori_loop(1, AHEAD, start, 0)

    def share_gain():
        @pl.when(ma // 2 == dev)
        def _():
            block = ma % 2
            pltpu.make_async_copy(gv, gs.at[block], gs_sem.at[block]).start()
            for step in range(1, 16):
                send(gv, gs.at[block], gs_out, gs_sem.at[block], {"dev": dev, "ma": (ma + step) % 16})

    def peaks(layer):
        @pl.when(layer == 0)
        def _():
            done(gs.at[0], gs_sem.at[0])
            done(gs.at[1], gs_sem.at[1])

        lane = lax.broadcasted_iota(jnp.int32, (192, 128), 1)
        for half in range(2):
            size = None
            for core in range(2):
                rows = sb[layer * 2 + core, place(layer * 2, half)].reshape(192, FEATS).astype(jnp.float32)
                rows = jnp.abs(rows * gs[core, pl.ds(layer, 1), :])
                rows = jnp.maximum(rows[:, :128], rows[:, 128:])
                size = rows if size is None else jnp.maximum(size, rows)
            top = jnp.max(size, axis=1, keepdims=True)
            part = slice(half * 192, (half + 1) * 192)
            pt[part, :] = jnp.where(lane == layer, top, pt[part, :])

        @pl.when(layer == LAYERS - 1)
        def _():
            for block in range(3):
                lanes = slice(block * 128, (block + 1) * 128)
                pt2[:, lanes] = jnp.transpose(pt[lanes, :])[0:LAYERS, :]

    def split_peaks():
        line = pt2[...]
        for group in range(8):
            part = pltpu.roll(line, COLS - group * PIECE, 1) if group else line
            pk0[group] = part[:, 0:128].astype(jnp.bfloat16)

    def send_peaks():
        pltpu.make_async_copy(pk0.at[dev], pk1.at[dev], pk1_sem).start()
        for step in range(1, 8):
            to = (dev + step) % 8
            send(pk0.at[to], pk1.at[dev], pk1_out, pk1_sem, {"dev": to, "ma": ma})

    def group_peaks():
        done(pk1, pk1_sem)
        pk2[ma] = jnp.max(pk1[...].astype(jnp.float32), axis=0).astype(jnp.bfloat16)

    def spread_peaks():
        for step in range(1, 16):
            send(pk2.at[ma], pk2.at[ma], pk2_out, pk2_sem, {"dev": dev, "ma": (ma + step) % 16})

    def last_peaks():
        done(pk2.at[0:15], pk2_sem)
        lane = lax.broadcasted_iota(jnp.int32, (LAYERS, 128), 1)
        for pair in range(PAIRS):
            halves = []
            for half in range(2):
                line = jnp.zeros((LAYERS, 128), jnp.float32)
                for piece in range(8):
                    shift = (piece - pair) * 16 % 128
                    part = pk2[half * 8 + piece].astype(jnp.float32)
                    part = pltpu.roll(part, shift, 1) if shift else part
                    line = jnp.where((lane >= piece * 16) & (lane < piece * 16 + 16), part, line)
                halves.append(line)
            low = jnp.where(zl == 1, halves[0], halves[1])
            high = jnp.where(zl == 1, halves[1], halves[0])
            line = jnp.concatenate([low, high], axis=1).astype(jnp.bfloat16)
            peak_ref[:, pair * 256 : (pair + 1) * 256] = lax.dot_general(
                line, rm[pair // 2], (((1,), (1,)), ((), ())), preferred_element_type=jnp.float32
            )

    def close(t):
        done(sb.at[t, 0:2, 0:3], y_out.at[t])

        @pl.when(t >= LATE)
        def _():
            done(sb.at[t, 2:4], first_out.at[t])

        @pl.when(t % 2 == c)
        def _():
            done(yb.at[t, :, 0:3], x_out.at[t])

        @pl.when(t % 2 != c)
        def _():
            done(yb.at[t], x_out.at[t])

    def turn(i, carry):
        def halves(at_step, stage, first, last):
            v = i - at_step

            @pl.when((v >= first) & (v < last))
            def _():
                stage(v // 2, v % 2)

        def chunks(at_step, stage, first, last):
            v = i - at_step

            @pl.when((v >= 2 * first) & (v < 2 * last) & (v % 2 == 0))
            def _():
                stage(v // 2)

        halves(0, along_x, 0, STEPS)
        pl.when(i <= CHUNKS - AHEAD)(lambda: first_send(i + AHEAD - 1))
        halves(-LEAD, along_y, 2 * LATE, STEPS)
        chunks(Z_FIRST_RELAY, lambda j: z_first_relay(LATE + j), 0, CHUNKS - LATE)
        halves(Z_LAST, lambda t, q: mine(t, lambda layer: z_last(layer, q)), 0, 2 * LATE)
        chunks(Z_LAST_RELAY, lambda t: mine(t, z_last_relay), 0, LATE)

        @pl.when(i < CHUNKS - AHEAD)
        def _():
            sort(i + AHEAD)

        chunks(FINISH_LATE, lambda t: mine(t, lambda layer: finish(layer, True)), 0, LATE)
        chunks(FINISH, lambda j: mine(LATE + j, lambda layer: finish(layer, False)), 0, CHUNKS - LATE)

        @pl.when((i >= PEAKS_FROM) & (i < PEAKS_FROM + LAYERS))
        def _():
            peaks(i - PEAKS_FROM)

        pl.when(i == PEAKS_SEND - 1)(split_peaks)
        pl.when(i == PEAKS_SEND)(send_peaks)
        pl.when(i == PEAKS_GROUP)(group_peaks)
        pl.when(i == PEAKS_SPREAD)(spread_peaks)
        pl.when(i == PEAKS_LAST)(last_peaks)

        chunks(CLOSE, close, 0, CHUNKS)
        pl.when(i == SHARE)(share_gain)
        pl.when(i == MATRIX)(lambda: order_matrix(rv, rm, zl))

        return carry

    lax.fori_loop(0, END, turn, 0)

    def close_layer(layer, carry):
        @pl.when(layer < LATE // 2)
        def _():
            done(gb.at[layer, 2:4], z_out.at[layer])

        return carry

    lax.fori_loop(0, LAYERS, close_layer, 0)

    @pl.when(ma // 2 == dev)
    def _():
        done(gs.at[0:15], gs_out)

    done(pk1.at[0:7], pk1_out)
    done(pk2.at[0:15], pk2_out)


def write_out(tiles_ref, peak_ref, q_ref, k_ref, v_ref, row_ref, sem):
    copies = [
        pltpu.make_async_copy(tiles_ref.at[:, pl.ds(0, 512)], q_ref, sem.at[0]),
        pltpu.make_async_copy(tiles_ref.at[:, pl.ds(512, 128)], k_ref, sem.at[1]),
        pltpu.make_async_copy(tiles_ref.at[:, pl.ds(640, 128)], v_ref, sem.at[2]),
        pltpu.make_async_copy(peak_ref, row_ref, sem.at[3]),
    ]
    for copy in copies:
        copy.start()
    for copy in copies:
        copy.wait()


def shards(joined_weight, norm_gain, rotary_order):
    dma = pltpu.SemaphoreType.DMA
    bf16, f32 = jnp.bfloat16, jnp.float32
    hbm = pl.BlockSpec(memory_space=pltpu.HBM)
    anywhere = pl.BlockSpec(memory_space=pl.ANY)
    tiles, peak = pl.pallas_call(
        kernel,
        name="relayout",
        out_shape=(jax.ShapeDtypeStruct((LAYERS, 768, FEATS), bf16), jax.ShapeDtypeStruct((LAYERS, 768), f32)),
        in_specs=[hbm, hbm, hbm],
        out_specs=(pl.BlockSpec(memory_space=pltpu.VMEM), pl.BlockSpec(memory_space=pltpu.VMEM)),
        scratch_shapes=[
            pltpu.VMEM((1, 128), jnp.int32),
            pltpu.VMEM((LAYERS, FEATS), f32),
            pltpu.VMEM((15, LAYERS, FEATS), f32),
            pltpu.VMEM((CHUNKS, FEATS, COLS), bf16),
            pltpu.VMEM((CHUNKS, 4, 4, PAIRS, 16, FEATS), bf16),
            pltpu.VMEM((CHUNKS, 2, 4, PAIRS, 16, FEATS), bf16),
            pltpu.VMEM((LAYERS, 4, 8, PAIRS, 16, FEATS), bf16),
            pltpu.VMEM((COLS, 128), f32),
            pltpu.VMEM((LAYERS, COLS), f32),
            pltpu.VMEM((8, LAYERS, 128), bf16),
            pltpu.VMEM((8, LAYERS, 128), bf16),
            pltpu.VMEM((16, LAYERS, 128), bf16),
            pltpu.VMEM((COLS, COLS), bf16),
            pltpu.VMEM((2, 256, 256), bf16),
            dma((CHUNKS,)),
            dma,
            dma,
            dma((2,)),
            dma,
            dma((CHUNKS,)),
            dma((CHUNKS,)),
            dma((CHUNKS * 2,)),
            dma((LAYERS * 2,)),
            dma((LAYERS * 2,)),
            dma((CHUNKS,)),
            dma((CHUNKS,)),
            dma((CHUNKS,)),
            dma((LAYERS,)),
            dma,
            dma,
            dma,
            dma,
        ],
        compiler_params=pltpu.CompilerParams(collective_id=0, has_side_effects=True, vmem_limit_bytes=40 * 2**20),
    )(*(pltpu.with_memory_space_constraint(a, pltpu.HBM) for a in (rotary_order.reshape(1, 128), norm_gain, joined_weight)))
    return pl.pallas_call(
        write_out,
        name="write_out",
        out_shape=(
            jax.ShapeDtypeStruct((LAYERS, 512, FEATS), bf16),
            jax.ShapeDtypeStruct((LAYERS, 128, FEATS), bf16),
            jax.ShapeDtypeStruct((LAYERS, 128, FEATS), bf16),
            jax.ShapeDtypeStruct((LAYERS, 768), f32),
        ),
        in_specs=[anywhere, anywhere],
        out_specs=(hbm, hbm, hbm, hbm),
        scratch_shapes=[dma((4,))],
        compiler_params=pltpu.CompilerParams(vmem_limit_bytes=2**20),
    )(tiles, peak)


def solution(mesh):
    placed = (P(None, "dev", "ma"), P(None, "ma"), P())
    tiles = P(None, "dev", "ma")
    return jax.shard_map(shards, mesh=mesh, in_specs=placed, out_specs=(tiles, tiles, tiles, P(None, "dev")), check_vma=False)
```

```python
import jax
import jax.numpy as jnp
from jax import lax
from jax.experimental import pallas as pl
from jax.experimental.pallas import tpu as pltpu
from jax.sharding import PartitionSpec as P

LAYERS = 8
CHUNKS = 16
FEATS = 256
COLS = 384
PIECE = 48
PAIRS = 3
LATE = 8
AHEAD = 8
LEAD = 5
SHARE, MATRIX, CLOSE = 0, 2, 5
STEPS = 2 * CHUNKS
Z_LAST, Z_LAST_RELAY, Z_FIRST_RELAY, FINISH_LATE, FINISH = 7, 18, 3, 23, 21
PEAKS_FROM, PEAKS_SEND, PEAKS_GROUP, PEAKS_SPREAD, PEAKS_LAST = 6, 15, 29, 30, 37
END = max(FINISH, FINISH_LATE) + 15
MESH = pl.DeviceIdType.MESH


def sort_matrix(pm_ref):
    row = lax.broadcasted_iota(jnp.int32, (COLS, 128), 0)
    lane = lax.broadcasted_iota(jnp.int32, (COLS, 128), 1)
    g = (row * 1366) >> 16
    rest = row - g * PIECE
    s, dd = rest >> 3, rest & 7
    head = jnp.where(s < 4, g * 4 + s, 32 + (s - 4) * 8 + g)
    column = dd * PIECE + head
    for block in range(COLS // 128):
        pm_ref[:, block * 128 : (block + 1) * 128] = jnp.where(column == lane + block * 128, 1.0, 0.0).astype(jnp.bfloat16)


def order_matrix(rot_ref, rm_ref, zl):
    turned = jnp.transpose(jnp.broadcast_to(rot_ref[0:1, :], (128, 128)))
    plain = lax.broadcasted_iota(jnp.int32, (128, 128), 0)
    lane = lax.broadcasted_iota(jnp.int32, (128, 128), 1)

    def hot(stored, s2, block):
        piece = stored >> 3
        half = piece >> 3
        slot = jnp.where(zl == 1, half, 1 - half)
        column = slot * 128 + (piece & 7) * 16 + s2 * 8 + (stored & 7)
        return jnp.where(column == lane + block * 128, 1.0, 0.0).astype(jnp.bfloat16)

    for block in range(2):
        lanes = slice(block * 128, (block + 1) * 128)
        key = hot(turned, 0, block)
        rm_ref[0, 0:128, lanes] = key
        rm_ref[1, 0:128, lanes] = key
        rm_ref[0, 128:256, lanes] = hot(turned, 1, block)
        rm_ref[1, 128:256, lanes] = hot(plain, 1, block)


def kernel(
    rot_ref, gain_ref, w_ref, out_ref, peak_ref,
    rv, gv, gs, xb, sb, yb, gb, pt, pt2, pk0, pk1, pk2, pm, rm,
    in_sem, rot_sem, gain_sem, gs_sem, gs_out, far_sem, near_sem, y_sem, x_sem, z_sem, first_out, y_out, x_out, z_out,
    pk1_sem, pk1_out, pk2_sem, pk2_out,
):
    dev, ma = lax.axis_index("dev"), lax.axis_index("ma")
    zh, y = dev // 4, dev % 4
    zl, x, c = ma // 8, (ma // 2) % 4, ma % 2
    z = zh * 2 + zl
    inner = (z == 1) | (z == 2)
    outer = (z == 0) | (z == 3)
    far_z = {"dev": (1 - zh) * 4 + y, "ma": (1 - zl) * 8 + x * 2 + c}
    near_z = {"dev": dev, "ma": (1 - zl) * 8 + x * 2 + c}

    def at(x_, y_, z_, c_):
        return {"dev": (z_ // 2) * 4 + y_, "ma": (z_ % 2) * 8 + x_ * 2 + c_}

    def send(src, dst, out_sem, in_sem_, device):
        pltpu.make_async_remote_copy(src, dst, out_sem, in_sem_, device_id=device, device_id_type=MESH).start()

    def done(ref, sem):
        pltpu.make_async_copy(ref, ref, sem).wait()

    def load(t):
        return pltpu.make_async_copy(w_ref.at[t // 2, pl.ds((1 - t % 2) * FEATS, FEATS), :], xb.at[t], in_sem.at[t])

    load_rot = pltpu.make_async_copy(rot_ref, rv, rot_sem)
    load_gain = pltpu.make_async_copy(gain_ref, gv, gain_sem)

    for n in range(CHUNKS):
        load(n // 2 + (n % 2) * LATE).start()
    load_rot.start()
    load_gain.start()

    barrier = pltpu.get_barrier_semaphore()
    for step in range(1, 16):
        pl.semaphore_signal(barrier, inc=1, device_id={"dev": dev, "ma": (ma + step) % 16}, device_id_type=MESH)
    for step in range(1, 8):
        pl.semaphore_signal(barrier, inc=1, device_id={"dev": (dev + step) % 8, "ma": ma}, device_id_type=MESH)
    pl.semaphore_signal(barrier, inc=1, device_id=far_z, device_id_type=MESH)

    def place(t, half):
        kept = zh == half
        early = jnp.where(kept, jnp.where(outer, 0, 3), 2)
        return jnp.where(t < LATE, jnp.where(kept, 0, 1), early)

    def sort(n):
        t = n // 2 + (n % 2) * LATE
        load(t).wait()
        rows = lax.dot_general(pm[...], xb[t], (((1,), (1,)), ((), ())), preferred_element_type=jnp.float32)
        rows = rows.astype(jnp.bfloat16).reshape(2, 4, PAIRS, 16, FEATS)
        sb[t, place(t, 0)] = rows[0]
        sb[t, place(t, 1)] = rows[1]

    def z_first(t):
        send(sb.at[t, 2], sb.at[t, jnp.where(outer, 3, 0)], first_out.at[t], far_sem.at[t], far_z)

        @pl.when(inner)
        def _():
            send(sb.at[t, 3], sb.at[t, 1], first_out.at[t], near_sem.at[t], near_z)

    def z_first_relay(t):
        @pl.when(outer)
        def _():
            done(sb.at[t, 3], far_sem.at[t])
            send(sb.at[t, 3], sb.at[t, 1], first_out.at[t], near_sem.at[t], near_z)

    def along_y(t, q):
        @pl.when((t >= LATE) & (q == 0) & inner)
        def _():
            done(sb.at[t, 0], far_sem.at[t])

        @pl.when((t >= LATE) & (q == 1))
        def _():
            done(sb.at[t, 1], near_sem.at[t])

        pltpu.make_async_copy(sb.at[t, q, y], yb.at[t, q, y], y_sem.at[t * 2 + q]).start()
        for step in (2, 1, 3):
            far = (y + step) % 4
            send(sb.at[t, q, far], yb.at[t, q, y], y_out.at[t], y_sem.at[t * 2 + q], at(x, far, z, c))

    def along_x(t, q):
        layer, core = t // 2, 1 - t % 2
        sent, sem = x_out.at[t], x_sem.at[layer * 2 + q]
        done(yb.at[t, q], y_sem.at[t * 2 + q])
        late = jnp.where(q == 1, 3, jnp.where(outer, 1, 2))
        slot = jnp.where(t < LATE, late, jnp.where(outer, 1 - q, q))
        target = gb.at[layer, slot, x * 2 + c]
        for step in (2, 1, 3):
            far = (x + step) % 4
            send(yb.at[t, q, far], target, sent, sem, at(far, y, z, core))

        @pl.when(core != c)
        def _():
            send(yb.at[t, q, x], target, sent, sem, at(x, y, z, 1 - c))

        @pl.when(core == c)
        def _():
            pltpu.make_async_copy(yb.at[t, q, x], target, sem).start()

    def mine(t, stage):
        @pl.when(t % 2 != c)
        def _():
            stage(t // 2)

    def z_last(layer, q):
        done(gb.at[layer, 2 + q], x_sem.at[layer * 2 + q])

        @pl.when(q == 1)
        def _():
            target = gb.at[layer, jnp.where(outer, 2, 0)]
            send(gb.at[layer, 3], target, z_out.at[layer], z_sem.at[layer * 2], far_z)

        @pl.when((q == 0) & inner)
        def _():
            send(gb.at[layer, 2], gb.at[layer, 0], z_out.at[layer], z_sem.at[layer * 2 + 1], near_z)

    def z_last_relay(layer):
        @pl.when(outer)
        def _():
            done(gb.at[layer, 2], z_sem.at[layer * 2])
            send(gb.at[layer, 2], gb.at[layer, 1], z_out.at[layer], z_sem.at[layer * 2 + 1], near_z)

    def finish(layer, late):
        if late:
            done(gb.at[layer, 0], z_sem.at[layer * 2 + 1])

            @pl.when(inner)
            def _():
                done(gb.at[layer, 1], z_sem.at[layer * 2])

        else:
            done(gb.at[layer, 0], x_sem.at[layer * 2])
            done(gb.at[layer, 1], x_sem.at[layer * 2 + 1])
        gain = gv[pl.ds(layer, 1), :]
        for pair in range(PAIRS):
            arrived = gb[layer, 0:2, :, pair].reshape(256, FEATS)
            rows = jnp.dot(rm[pair // 2], arrived, preferred_element_type=jnp.float32) * gain
            out_ref[layer, pair * 256 : (pair + 1) * 256, :] = rows.astype(jnp.bfloat16)

    def first_send(n):
        @pl.when(n % 2 == 0)
        def _():
            along_y(n // 2, 0)
            along_y(n // 2, 1)

        @pl.when(n % 2 == 1)
        def _():
            z_first(LATE + n // 2)

    def start(n, carry):
        sort(n)
        first_send(n - 1)
        return carry

    sort_matrix(pm)
    sort(0)
    load_gain.wait()
    load_rot.wait()
    pl.semaphore_wait(barrier, 23)
    lax.fori_loop(1, AHEAD, start, 0)

    def share_gain():
        @pl.when(ma // 2 == dev)
        def _():
            block = ma % 2
            pltpu.make_async_copy(gv, gs.at[block], gs_sem.at[block]).start()
            for step in range(1, 16):
                send(gv, gs.at[block], gs_out, gs_sem.at[block], {"dev": dev, "ma": (ma + step) % 16})

    def peaks(layer):
        @pl.when(layer == 0)
        def _():
            done(gs.at[0], gs_sem.at[0])
            done(gs.at[1], gs_sem.at[1])

        lane = lax.broadcasted_iota(jnp.int32, (192, 128), 1)
        for half in range(2):
            size = None
            for core in range(2):
                rows = sb[layer * 2 + core, place(layer * 2, half)].reshape(192, FEATS).astype(jnp.float32)
                rows = jnp.abs(rows * gs[1 - core, pl.ds(layer, 1), :])
                rows = jnp.maximum(rows[:, :128], rows[:, 128:])
                size = rows if size is None else jnp.maximum(size, rows)
            top = jnp.max(size, axis=1, keepdims=True)
            part = slice(half * 192, (half + 1) * 192)
            pt[part, :] = jnp.where(lane == layer, top, pt[part, :])

        @pl.when(layer == LAYERS - 1)
        def _():
            for block in range(3):
                lanes = slice(block * 128, (block + 1) * 128)
                pt2[:, lanes] = jnp.transpose(pt[lanes, :])[0:LAYERS, :]

    def split_peaks():
        line = pt2[...]
        for group in range(8):
            part = pltpu.roll(line, COLS - group * PIECE, 1) if group else line
            pk0[group] = part[:, 0:128].astype(jnp.bfloat16)

    def send_peaks():
        pltpu.make_async_copy(pk0.at[dev], pk1.at[dev], pk1_sem).start()
        for step in range(1, 8):
            to = (dev + step) % 8
            send(pk0.at[to], pk1.at[dev], pk1_out, pk1_sem, {"dev": to, "ma": ma})

    def group_peaks():
        done(pk1, pk1_sem)
        pk2[ma] = jnp.max(pk1[...].astype(jnp.float32), axis=0).astype(jnp.bfloat16)

    def spread_peaks():
        for step in range(1, 16):
            send(pk2.at[ma], pk2.at[ma], pk2_out, pk2_sem, {"dev": dev, "ma": (ma + step) % 16})

    def last_peaks():
        done(pk2.at[0:15], pk2_sem)
        lane = lax.broadcasted_iota(jnp.int32, (LAYERS, 128), 1)
        for pair in range(PAIRS):
            halves = []
            for half in range(2):
                line = jnp.zeros((LAYERS, 128), jnp.float32)
                for piece in range(8):
                    shift = (piece - pair) * 16 % 128
                    part = pk2[half * 8 + piece].astype(jnp.float32)
                    part = pltpu.roll(part, shift, 1) if shift else part
                    line = jnp.where((lane >= piece * 16) & (lane < piece * 16 + 16), part, line)
                halves.append(line)
            low = jnp.where(zl == 1, halves[0], halves[1])
            high = jnp.where(zl == 1, halves[1], halves[0])
            line = jnp.concatenate([low, high], axis=1).astype(jnp.bfloat16)
            peak_ref[:, pair * 256 : (pair + 1) * 256] = lax.dot_general(
                line, rm[pair // 2], (((1,), (1,)), ((), ())), preferred_element_type=jnp.float32
            )

    def close(t):
        done(sb.at[t, 0:2, 0:3], y_out.at[t])

        @pl.when(t >= LATE)
        def _():
            done(sb.at[t, 2:4], first_out.at[t])

        @pl.when(t % 2 != c)
        def _():
            done(yb.at[t, :, 0:3], x_out.at[t])

        @pl.when(t % 2 == c)
        def _():
            done(yb.at[t], x_out.at[t])

    def turn(i, carry):
        def halves(at_step, stage, first, last):
            v = i - at_step

            @pl.when((v >= first) & (v < last))
            def _():
                stage(v // 2, v % 2)

        def chunks(at_step, stage, first, last):
            v = i - at_step

            @pl.when((v >= 2 * first) & (v < 2 * last) & (v % 2 == 0))
            def _():
                stage(v // 2)

        halves(0, along_x, 0, STEPS)
        pl.when(i <= CHUNKS - AHEAD)(lambda: first_send(i + AHEAD - 1))
        halves(-LEAD, along_y, 2 * LATE, STEPS)
        chunks(Z_FIRST_RELAY, lambda j: z_first_relay(LATE + j), 0, CHUNKS - LATE)
        halves(Z_LAST, lambda t, q: mine(t, lambda layer: z_last(layer, q)), 0, 2 * LATE)
        chunks(Z_LAST_RELAY, lambda t: mine(t, z_last_relay), 0, LATE)

        @pl.when(i < CHUNKS - AHEAD)
        def _():
            sort(i + AHEAD)

        chunks(FINISH_LATE, lambda t: mine(t, lambda layer: finish(layer, True)), 0, LATE)
        chunks(FINISH, lambda j: mine(LATE + j, lambda layer: finish(layer, False)), 0, CHUNKS - LATE)

        @pl.when((i >= PEAKS_FROM) & (i < PEAKS_FROM + LAYERS))
        def _():
            peaks(i - PEAKS_FROM)

        pl.when(i == PEAKS_SEND - 1)(split_peaks)
        pl.when(i == PEAKS_SEND)(send_peaks)
        pl.when(i == PEAKS_GROUP)(group_peaks)
        pl.when(i == PEAKS_SPREAD)(spread_peaks)
        pl.when(i == PEAKS_LAST)(last_peaks)

        chunks(CLOSE, close, 0, CHUNKS)
        pl.when(i == SHARE)(share_gain)
        pl.when(i == MATRIX)(lambda: order_matrix(rv, rm, zl))

        return carry

    lax.fori_loop(0, END, turn, 0)

    def close_layer(layer, carry):
        @pl.when(layer < LATE // 2)
        def _():
            done(gb.at[layer, 2:4], z_out.at[layer])

        return carry

    lax.fori_loop(0, LAYERS, close_layer, 0)

    @pl.when(ma // 2 == dev)
    def _():
        done(gs.at[0:15], gs_out)

    done(pk1.at[0:7], pk1_out)
    done(pk2.at[0:15], pk2_out)


def write_out(tiles_ref, peak_ref, q_ref, k_ref, v_ref, row_ref, sem):
    copies = [
        pltpu.make_async_copy(tiles_ref.at[:, pl.ds(0, 512)], q_ref, sem.at[0]),
        pltpu.make_async_copy(tiles_ref.at[:, pl.ds(512, 128)], k_ref, sem.at[1]),
        pltpu.make_async_copy(tiles_ref.at[:, pl.ds(640, 128)], v_ref, sem.at[2]),
        pltpu.make_async_copy(peak_ref, row_ref, sem.at[3]),
    ]
    for copy in copies:
        copy.start()
    for copy in copies:
        copy.wait()


def shards(joined_weight, norm_gain, rotary_order):
    dma = pltpu.SemaphoreType.DMA
    bf16, f32 = jnp.bfloat16, jnp.float32
    hbm = pl.BlockSpec(memory_space=pltpu.HBM)
    anywhere = pl.BlockSpec(memory_space=pl.ANY)
    tiles, peak = pl.pallas_call(
        kernel,
        name="relayout",
        out_shape=(jax.ShapeDtypeStruct((LAYERS, 768, FEATS), bf16), jax.ShapeDtypeStruct((LAYERS, 768), f32)),
        in_specs=[hbm, hbm, hbm],
        out_specs=(pl.BlockSpec(memory_space=pltpu.VMEM), pl.BlockSpec(memory_space=pltpu.VMEM)),
        scratch_shapes=[
            pltpu.VMEM((1, 128), jnp.int32),
            pltpu.VMEM((LAYERS, FEATS), f32),
            pltpu.VMEM((15, LAYERS, FEATS), f32),
            pltpu.VMEM((CHUNKS, FEATS, COLS), bf16),
            pltpu.VMEM((CHUNKS, 4, 4, PAIRS, 16, FEATS), bf16),
            pltpu.VMEM((CHUNKS, 2, 4, PAIRS, 16, FEATS), bf16),
            pltpu.VMEM((LAYERS, 4, 8, PAIRS, 16, FEATS), bf16),
            pltpu.VMEM((COLS, 128), f32),
            pltpu.VMEM((LAYERS, COLS), f32),
            pltpu.VMEM((8, LAYERS, 128), bf16),
            pltpu.VMEM((8, LAYERS, 128), bf16),
            pltpu.VMEM((16, LAYERS, 128), bf16),
            pltpu.VMEM((COLS, COLS), bf16),
            pltpu.VMEM((2, 256, 256), bf16),
            dma((CHUNKS,)),
            dma,
            dma,
            dma((2,)),
            dma,
            dma((CHUNKS,)),
            dma((CHUNKS,)),
            dma((CHUNKS * 2,)),
            dma((LAYERS * 2,)),
            dma((LAYERS * 2,)),
            dma((CHUNKS,)),
            dma((CHUNKS,)),
            dma((CHUNKS,)),
            dma((LAYERS,)),
            dma,
            dma,
            dma,
            dma,
        ],
        compiler_params=pltpu.CompilerParams(collective_id=0, has_side_effects=True, vmem_limit_bytes=40 * 2**20),
    )(*(pltpu.with_memory_space_constraint(a, pltpu.HBM) for a in (rotary_order.reshape(1, 128), norm_gain, joined_weight)))
    return pl.pallas_call(
        write_out,
        name="write_out",
        out_shape=(
            jax.ShapeDtypeStruct((LAYERS, 512, FEATS), bf16),
            jax.ShapeDtypeStruct((LAYERS, 128, FEATS), bf16),
            jax.ShapeDtypeStruct((LAYERS, 128, FEATS), bf16),
            jax.ShapeDtypeStruct((LAYERS, 768), f32),
        ),
        in_specs=[anywhere, anywhere],
        out_specs=(hbm, hbm, hbm, hbm),
        scratch_shapes=[dma((4,))],
        compiler_params=pltpu.CompilerParams(vmem_limit_bytes=2**20),
    )(tiles, peak)


def solution(mesh):
    placed = (P(None, "dev", "ma"), P(None, "ma"), P())
    tiles = P(None, "dev", "ma")
    return jax.shard_map(shards, mesh=mesh, in_specs=placed, out_specs=(tiles, tiles, tiles, P(None, "dev")), check_vma=False)
```

```python
import jax
import jax.numpy as jnp
from jax import lax
from jax.experimental import pallas as pl
from jax.experimental.pallas import tpu as pltpu
from jax.sharding import PartitionSpec as P

LAYERS = 8
CHUNKS = 16
FEATS = 256
COLS = 384
PIECE = 48
PAIRS = 3
LATE = 8
AHEAD = 8
LEAD = 5
SHARE, MATRIX, CLOSE = 0, 2, 5
STEPS = 2 * CHUNKS
Z_LAST, Z_LAST_RELAY, Z_FIRST_RELAY, FINISH_LATE, FINISH = 7, 18, 3, 23, 21
PEAKS_FROM, PEAKS_SEND, PEAKS_GROUP, PEAKS_SPREAD, PEAKS_LAST = 6, 15, 28, 29, 36
END = max(FINISH, FINISH_LATE) + 15
MESH = pl.DeviceIdType.MESH


def sort_matrix(pm_ref):
    row = lax.broadcasted_iota(jnp.int32, (COLS, 128), 0)
    lane = lax.broadcasted_iota(jnp.int32, (COLS, 128), 1)
    g = (row * 1366) >> 16
    rest = row - g * PIECE
    s, dd = rest >> 3, rest & 7
    head = jnp.where(s < 4, g * 4 + s, 32 + (s - 4) * 8 + g)
    column = dd * PIECE + head
    for block in range(COLS // 128):
        pm_ref[:, block * 128 : (block + 1) * 128] = jnp.where(column == lane + block * 128, 1.0, 0.0).astype(jnp.bfloat16)


def order_matrix(rot_ref, rm_ref, zl):
    turned = jnp.transpose(jnp.broadcast_to(rot_ref[0:1, :], (128, 128)))
    plain = lax.broadcasted_iota(jnp.int32, (128, 128), 0)
    lane = lax.broadcasted_iota(jnp.int32, (128, 128), 1)

    def hot(stored, s2, block):
        piece = stored >> 3
        half = piece >> 3
        slot = jnp.where(zl == 1, half, 1 - half)
        column = slot * 128 + (piece & 7) * 16 + s2 * 8 + (stored & 7)
        return jnp.where(column == lane + block * 128, 1.0, 0.0).astype(jnp.bfloat16)

    for block in range(2):
        lanes = slice(block * 128, (block + 1) * 128)
        key = hot(turned, 0, block)
        rm_ref[0, 0:128, lanes] = key
        rm_ref[1, 0:128, lanes] = key
        rm_ref[0, 128:256, lanes] = hot(turned, 1, block)
        rm_ref[1, 128:256, lanes] = hot(plain, 1, block)


def serve(gb, rm, gv, layer, out_ref, place):
    gain = gv[pl.ds(layer, 1), :]
    for pair in range(PAIRS):
        arrived = gb[layer, 0:2, :, pair].reshape(256, FEATS)
        rows = jnp.dot(rm[pair // 2], arrived, preferred_element_type=jnp.float32) * gain
        out_ref[place, pair * 256 : (pair + 1) * 256, :] = rows.astype(jnp.bfloat16)


def kernel(
    rot_ref, gain_ref, w_ref, out_ref, peak_ref, gb, rm, gv,
    rv, gs, xb, sb, yb, pt, pt2, pk0, pk1, pk2, pm,
    in_sem, rot_sem, gain_sem, gs_sem, gs_out, far_sem, near_sem, y_sem, x_sem, z_sem, first_out, y_out, x_out, z_out,
    pk1_sem, pk1_out, pk2_sem, pk2_out,
):
    dev, ma = lax.axis_index("dev"), lax.axis_index("ma")
    zh, y = dev // 4, dev % 4
    zl, x, c = ma // 8, (ma // 2) % 4, ma % 2
    z = zh * 2 + zl
    inner = (z == 1) | (z == 2)
    outer = (z == 0) | (z == 3)
    far_z = {"dev": (1 - zh) * 4 + y, "ma": (1 - zl) * 8 + x * 2 + c}
    near_z = {"dev": dev, "ma": (1 - zl) * 8 + x * 2 + c}

    def at(x_, y_, z_, c_):
        return {"dev": (z_ // 2) * 4 + y_, "ma": (z_ % 2) * 8 + x_ * 2 + c_}

    def send(src, dst, out_sem, in_sem_, device):
        pltpu.make_async_remote_copy(src, dst, out_sem, in_sem_, device_id=device, device_id_type=MESH).start()

    def done(ref, sem):
        pltpu.make_async_copy(ref, ref, sem).wait()

    def load(t):
        return pltpu.make_async_copy(w_ref.at[t // 2, pl.ds((1 - t % 2) * FEATS, FEATS), :], xb.at[t], in_sem.at[t])

    load_rot = pltpu.make_async_copy(rot_ref, rv, rot_sem)
    load_gain = pltpu.make_async_copy(gain_ref, gv, gain_sem)

    for n in range(CHUNKS):
        load(n // 2 + (n % 2) * LATE).start()
    load_rot.start()
    load_gain.start()

    barrier = pltpu.get_barrier_semaphore()
    for step in range(1, 16):
        pl.semaphore_signal(barrier, inc=1, device_id={"dev": dev, "ma": (ma + step) % 16}, device_id_type=MESH)
    for step in range(1, 8):
        pl.semaphore_signal(barrier, inc=1, device_id={"dev": (dev + step) % 8, "ma": ma}, device_id_type=MESH)
    pl.semaphore_signal(barrier, inc=1, device_id=far_z, device_id_type=MESH)

    def place(t, half):
        kept = zh == half
        early = jnp.where(kept, jnp.where(outer, 0, 3), 2)
        return jnp.where(t < LATE, jnp.where(kept, 0, 1), early)

    def sort(n):
        t = n // 2 + (n % 2) * LATE
        load(t).wait()
        rows = lax.dot_general(pm[...], xb[t], (((1,), (1,)), ((), ())), preferred_element_type=jnp.float32)
        rows = rows.astype(jnp.bfloat16).reshape(2, 4, PAIRS, 16, FEATS)
        sb[t, place(t, 0)] = rows[0]
        sb[t, place(t, 1)] = rows[1]

    def z_first(t):
        send(sb.at[t, 2], sb.at[t, jnp.where(outer, 3, 0)], first_out.at[t], far_sem.at[t], far_z)

        @pl.when(inner)
        def _():
            send(sb.at[t, 3], sb.at[t, 1], first_out.at[t], near_sem.at[t], near_z)

    def z_first_relay(t):
        @pl.when(outer)
        def _():
            done(sb.at[t, 3], far_sem.at[t])
            send(sb.at[t, 3], sb.at[t, 1], first_out.at[t], near_sem.at[t], near_z)

    def along_y(t, q):
        @pl.when((t >= LATE) & (q == 0) & inner)
        def _():
            done(sb.at[t, 0], far_sem.at[t])

        @pl.when((t >= LATE) & (q == 1))
        def _():
            done(sb.at[t, 1], near_sem.at[t])

        pltpu.make_async_copy(sb.at[t, q, y], yb.at[t, q, y], y_sem.at[t * 2 + q]).start()
        for step in (2, 1, 3):
            far = (y + step) % 4
            send(sb.at[t, q, far], yb.at[t, q, y], y_out.at[t], y_sem.at[t * 2 + q], at(x, far, z, c))

    def along_x(t, q):
        layer, core = t // 2, 1 - t % 2
        sent, sem = x_out.at[t], x_sem.at[layer * 2 + q]
        done(yb.at[t, q], y_sem.at[t * 2 + q])
        late = jnp.where(q == 1, 3, jnp.where(outer, 1, 2))
        slot = jnp.where(t < LATE, late, jnp.where(outer, 1 - q, q))
        target = gb.at[layer, slot, x * 2 + c]
        for step in (2, 1, 3):
            far = (x + step) % 4
            send(yb.at[t, q, far], target, sent, sem, at(far, y, z, core))

        @pl.when(core != c)
        def _():
            send(yb.at[t, q, x], target, sent, sem, at(x, y, z, 1 - c))

        @pl.when(core == c)
        def _():
            pltpu.make_async_copy(yb.at[t, q, x], target, sem).start()

    def mine(t, stage):
        @pl.when(t % 2 != c)
        def _():
            stage(t // 2)

    def z_last(layer, q):
        done(gb.at[layer, 2 + q], x_sem.at[layer * 2 + q])

        @pl.when(q == 1)
        def _():
            target = gb.at[layer, jnp.where(outer, 2, 0)]
            send(gb.at[layer, 3], target, z_out.at[layer], z_sem.at[layer * 2], far_z)

        @pl.when((q == 0) & inner)
        def _():
            send(gb.at[layer, 2], gb.at[layer, 0], z_out.at[layer], z_sem.at[layer * 2 + 1], near_z)

    def z_last_relay(layer):
        @pl.when(outer)
        def _():
            done(gb.at[layer, 2], z_sem.at[layer * 2])
            send(gb.at[layer, 2], gb.at[layer, 1], z_out.at[layer], z_sem.at[layer * 2 + 1], near_z)

    def finish(layer, late):
        if late:
            done(gb.at[layer, 0], z_sem.at[layer * 2 + 1])

            @pl.when(inner)
            def _():
                done(gb.at[layer, 1], z_sem.at[layer * 2])

        else:
            done(gb.at[layer, 0], x_sem.at[layer * 2])
            done(gb.at[layer, 1], x_sem.at[layer * 2 + 1])

        @pl.when(layer != (LATE // 2 if late else LAYERS) - 1)
        def _():
            serve(gb, rm, gv, layer, out_ref, layer)

    def first_send(n):
        @pl.when(n % 2 == 0)
        def _():
            along_y(n // 2, 0)
            along_y(n // 2, 1)

        @pl.when(n % 2 == 1)
        def _():
            z_first(LATE + n // 2)

    def start(n, carry):
        sort(n)
        first_send(n - 1)
        return carry

    sort_matrix(pm)
    sort(0)
    pl.semaphore_wait(barrier, 23)
    lax.fori_loop(1, AHEAD, start, 0)
    load_gain.wait()
    load_rot.wait()

    def share_gain():
        @pl.when(ma // 2 == dev)
        def _():
            block = ma % 2
            pltpu.make_async_copy(gv, gs.at[block], gs_sem.at[block]).start()
            for step in range(1, 16):
                send(gv, gs.at[block], gs_out, gs_sem.at[block], {"dev": dev, "ma": (ma + step) % 16})

    def peaks(layer):
        @pl.when(layer == 0)
        def _():
            done(gs.at[0], gs_sem.at[0])
            done(gs.at[1], gs_sem.at[1])

        lane = lax.broadcasted_iota(jnp.int32, (192, 128), 1)
        for half in range(2):
            size = None
            for core in range(2):
                rows = sb[layer * 2 + core, place(layer * 2, half)].reshape(192, FEATS).astype(jnp.float32)
                rows = jnp.abs(rows * gs[1 - core, pl.ds(layer, 1), :])
                rows = jnp.maximum(rows[:, :128], rows[:, 128:])
                size = rows if size is None else jnp.maximum(size, rows)
            top = jnp.max(size, axis=1, keepdims=True)
            part = slice(half * 192, (half + 1) * 192)
            pt[part, :] = jnp.where(lane == layer, top, pt[part, :])

        @pl.when(layer == LAYERS - 1)
        def _():
            for block in range(3):
                lanes = slice(block * 128, (block + 1) * 128)
                pt2[:, lanes] = jnp.transpose(pt[lanes, :])[0:LAYERS, :]

    def split_peaks():
        line = pt2[...]
        for group in range(8):
            part = pltpu.roll(line, COLS - group * PIECE, 1) if group else line
            pk0[group] = part[:, 0:128].astype(jnp.bfloat16)

    def send_peaks():
        pltpu.make_async_copy(pk0.at[dev], pk1.at[dev], pk1_sem).start()
        for step in range(1, 8):
            to = (dev + step) % 8
            send(pk0.at[to], pk1.at[dev], pk1_out, pk1_sem, {"dev": to, "ma": ma})

    def group_peaks():
        done(pk1, pk1_sem)
        pk2[ma] = jnp.max(pk1[...].astype(jnp.float32), axis=0).astype(jnp.bfloat16)

    def spread_peaks():
        for step in range(1, 16):
            send(pk2.at[ma], pk2.at[ma], pk2_out, pk2_sem, {"dev": dev, "ma": (ma + step) % 16})

    def last_peaks():
        done(pk2.at[0:15], pk2_sem)
        lane = lax.broadcasted_iota(jnp.int32, (LAYERS, 128), 1)
        for pair in range(PAIRS):
            halves = []
            for half in range(2):
                line = jnp.zeros((LAYERS, 128), jnp.float32)
                for piece in range(8):
                    shift = (piece - pair) * 16 % 128
                    part = pk2[half * 8 + piece].astype(jnp.float32)
                    part = pltpu.roll(part, shift, 1) if shift else part
                    line = jnp.where((lane >= piece * 16) & (lane < piece * 16 + 16), part, line)
                halves.append(line)
            low = jnp.where(zl == 1, halves[0], halves[1])
            high = jnp.where(zl == 1, halves[1], halves[0])
            line = jnp.concatenate([low, high], axis=1).astype(jnp.bfloat16)
            peak_ref[:, pair * 256 : (pair + 1) * 256] = lax.dot_general(
                line, rm[pair // 2], (((1,), (1,)), ((), ())), preferred_element_type=jnp.float32
            )

    def close(t):
        done(sb.at[t, 0:2, 0:3], y_out.at[t])

        @pl.when(t >= LATE)
        def _():
            done(sb.at[t, 2:4], first_out.at[t])

        @pl.when(t % 2 != c)
        def _():
            done(yb.at[t, :, 0:3], x_out.at[t])

        @pl.when(t % 2 == c)
        def _():
            done(yb.at[t], x_out.at[t])

    def turn(i, carry):
        def halves(at_step, stage, first, last):
            v = i - at_step

            @pl.when((v >= first) & (v < last))
            def _():
                stage(v // 2, v % 2)

        def chunks(at_step, stage, first, last):
            v = i - at_step

            @pl.when((v >= 2 * first) & (v < 2 * last) & (v % 2 == 0))
            def _():
                stage(v // 2)

        halves(0, along_x, 0, STEPS)
        pl.when(i <= CHUNKS - AHEAD)(lambda: first_send(i + AHEAD - 1))
        halves(-LEAD, along_y, 2 * LATE, STEPS)
        chunks(Z_FIRST_RELAY, lambda j: z_first_relay(LATE + j), 0, CHUNKS - LATE)
        halves(Z_LAST, lambda t, q: mine(t, lambda layer: z_last(layer, q)), 0, 2 * LATE)
        chunks(Z_LAST_RELAY, lambda t: mine(t, z_last_relay), 0, LATE)

        @pl.when(i < CHUNKS - AHEAD)
        def _():
            sort(i + AHEAD)

        chunks(FINISH_LATE, lambda t: mine(t, lambda layer: finish(layer, True)), 0, LATE)
        chunks(FINISH, lambda j: mine(LATE + j, lambda layer: finish(layer, False)), 0, CHUNKS - LATE)

        @pl.when((i >= PEAKS_FROM) & (i < PEAKS_FROM + LAYERS))
        def _():
            peaks(i - PEAKS_FROM)

        pl.when(i == PEAKS_SEND - 1)(split_peaks)
        pl.when(i == PEAKS_SEND)(send_peaks)
        pl.when(i == PEAKS_GROUP)(group_peaks)
        pl.when(i == PEAKS_SPREAD)(spread_peaks)
        pl.when(i == PEAKS_LAST)(last_peaks)

        chunks(CLOSE, close, 0, CHUNKS)
        pl.when(i == SHARE)(share_gain)
        pl.when(i == MATRIX)(lambda: order_matrix(rv, rm, zl))

        return carry

    lax.fori_loop(0, END, turn, 0)

    def close_layer(layer, carry):
        @pl.when(layer < LATE // 2)
        def _():
            done(gb.at[layer, 2:4], z_out.at[layer])

        return carry

    lax.fori_loop(0, LAYERS, close_layer, 0)

    @pl.when(ma // 2 == dev)
    def _():
        done(gs.at[0:15], gs_out)

    done(pk1.at[0:7], pk1_out)
    done(pk2.at[0:15], pk2_out)


def write_out(tiles_ref, peak_ref, gb, rm, gv, q_ref, k_ref, v_ref, row_ref, last, sem):
    copies = []

    def copy(src, dst):
        copies.append(pltpu.make_async_copy(src, dst, sem.at[len(copies)]))
        copies[-1].start()

    def tiles(src, layers):
        for out, first, count in ((q_ref, 0, 512), (k_ref, 512, 128), (v_ref, 640, 128)):
            copy(src.at[:, pl.ds(first, count)], out.at[layers])

    half = LATE // 2
    for layers in (pl.ds(0, half - 1), pl.ds(half, LAYERS - half - 1)):
        tiles(tiles_ref.at[layers], layers)
    copy(peak_ref, row_ref)
    for place, layer in enumerate((half - 1, LAYERS - 1)):
        serve(gb, rm, gv, layer, last, place)
        tiles(last.at[pl.ds(place, 1)], pl.ds(layer, 1))
    for waited in copies:
        waited.wait()


def shards(joined_weight, norm_gain, rotary_order):
    dma = pltpu.SemaphoreType.DMA
    bf16, f32 = jnp.bfloat16, jnp.float32
    hbm = pl.BlockSpec(memory_space=pltpu.HBM)
    vmem = pl.BlockSpec(memory_space=pltpu.VMEM)
    moved = pl.pallas_call(
        kernel,
        name="relayout",
        out_shape=(
            jax.ShapeDtypeStruct((LAYERS, 768, FEATS), bf16),
            jax.ShapeDtypeStruct((LAYERS, 768), f32),
            jax.ShapeDtypeStruct((LAYERS, 4, 8, PAIRS, 16, FEATS), bf16),
            jax.ShapeDtypeStruct((2, 256, 256), bf16),
            jax.ShapeDtypeStruct((LAYERS, FEATS), f32),
        ),
        in_specs=[hbm, hbm, hbm],
        out_specs=(vmem,) * 5,
        scratch_shapes=[
            pltpu.VMEM((1, 128), jnp.int32),
            pltpu.VMEM((15, LAYERS, FEATS), f32),
            pltpu.VMEM((CHUNKS, FEATS, COLS), bf16),
            pltpu.VMEM((CHUNKS, 4, 4, PAIRS, 16, FEATS), bf16),
            pltpu.VMEM((CHUNKS, 2, 4, PAIRS, 16, FEATS), bf16),
            pltpu.VMEM((COLS, 128), f32),
            pltpu.VMEM((LAYERS, COLS), f32),
            pltpu.VMEM((8, LAYERS, 128), bf16),
            pltpu.VMEM((8, LAYERS, 128), bf16),
            pltpu.VMEM((16, LAYERS, 128), bf16),
            pltpu.VMEM((COLS, COLS), bf16),
            dma((CHUNKS,)),
            dma,
            dma,
            dma((2,)),
            dma,
            dma((CHUNKS,)),
            dma((CHUNKS,)),
            dma((CHUNKS * 2,)),
            dma((LAYERS * 2,)),
            dma((LAYERS * 2,)),
            dma((CHUNKS,)),
            dma((CHUNKS,)),
            dma((CHUNKS,)),
            dma((LAYERS,)),
            dma,
            dma,
            dma,
            dma,
        ],
        compiler_params=pltpu.CompilerParams(collective_id=0, has_side_effects=True, vmem_limit_bytes=40 * 2**20),
    )(*(pltpu.with_memory_space_constraint(a, pltpu.HBM) for a in (rotary_order.reshape(1, 128), norm_gain, joined_weight)))
    return pl.pallas_call(
        write_out,
        name="write_out",
        out_shape=(
            jax.ShapeDtypeStruct((LAYERS, 512, FEATS), bf16),
            jax.ShapeDtypeStruct((LAYERS, 128, FEATS), bf16),
            jax.ShapeDtypeStruct((LAYERS, 128, FEATS), bf16),
            jax.ShapeDtypeStruct((LAYERS, 768), f32),
        ),
        in_specs=[vmem] * 5,
        out_specs=(hbm, hbm, hbm, hbm),
        scratch_shapes=[pltpu.VMEM((2, 768, FEATS), bf16), dma((13,))],
        compiler_params=pltpu.CompilerParams(vmem_limit_bytes=4 * 2**20),
    )(*moved)


def solution(mesh):
    placed = (P(None, "dev", "ma"), P(None, "ma"), P())
    tiles = P(None, "dev", "ma")
    return jax.shard_map(shards, mesh=mesh, in_specs=placed, out_specs=(tiles, tiles, tiles, P(None, "dev")), check_vma=False)
```

```python
import jax
import jax.numpy as jnp
from jax import lax
from jax.experimental import pallas as pl
from jax.experimental.pallas import tpu as pltpu
from jax.sharding import PartitionSpec as P

LAYERS = 8
CHUNKS = 16
FEATS = 256
COLS = 384
PIECE = 48
PAIRS = 3
LATE = 8
AHEAD = 10
LEAD = 5
SHARE, MATRIX, CLOSE = 0, 2, 5
STEPS = 2 * CHUNKS
Z_LAST, Z_LAST_RELAY, Z_FIRST_RELAY, FINISH_LATE, FINISH = 7, 17, 3, 23, 21
PEAKS_FROM, PEAKS_SEND, PEAKS_GROUP, PEAKS_SPREAD = 6, 15, 27, 28
END = max(FINISH, FINISH_LATE) + 15
MESH = pl.DeviceIdType.MESH


def sort_matrix(pm_ref):
    row = lax.broadcasted_iota(jnp.int32, (COLS, 128), 0)
    lane = lax.broadcasted_iota(jnp.int32, (COLS, 128), 1)
    g = (row * 1366) >> 16
    rest = row - g * PIECE
    s, dd = rest >> 3, rest & 7
    head = jnp.where(s < 4, g * 4 + s, 32 + (s - 4) * 8 + g)
    column = dd * PIECE + head
    for block in range(COLS // 128):
        pm_ref[:, block * 128 : (block + 1) * 128] = jnp.where(column == lane + block * 128, 1.0, 0.0).astype(jnp.bfloat16)


def order_matrix(rot_ref, rm_ref, zl):
    turned = jnp.transpose(jnp.broadcast_to(rot_ref[0:1, :], (128, 128)))
    plain = lax.broadcasted_iota(jnp.int32, (128, 128), 0)
    lane = lax.broadcasted_iota(jnp.int32, (128, 128), 1)

    def hot(stored, s2, block):
        piece = stored >> 3
        half = piece >> 3
        slot = jnp.where(zl == 1, half, 1 - half)
        column = slot * 128 + (piece & 7) * 16 + s2 * 8 + (stored & 7)
        return jnp.where(column == lane + block * 128, 1.0, 0.0).astype(jnp.bfloat16)

    for block in range(2):
        lanes = slice(block * 128, (block + 1) * 128)
        key = hot(turned, 0, block)
        rm_ref[0, 0:128, lanes] = key
        rm_ref[1, 0:128, lanes] = key
        rm_ref[0, 128:256, lanes] = hot(turned, 1, block)
        rm_ref[1, 128:256, lanes] = hot(plain, 1, block)


def serve(gb, rm, gv, layer, out_ref, place):
    gain = gv[pl.ds(layer, 1), :]
    for pair in range(PAIRS):
        arrived = gb[layer, 0:2, :, pair].reshape(256, FEATS)
        rows = jnp.dot(rm[pair // 2], arrived, preferred_element_type=jnp.float32) * gain
        out_ref[place, pair * 256 : (pair + 1) * 256, :] = rows.astype(jnp.bfloat16)


def kernel(
    rot_ref, gain_ref, w_ref, out_ref, pk3, gb, rm, gv,
    rv, gs, xb, sb, yb, pt, pt2, pk0, pk1, pk2, pm,
    in_sem, rot_sem, gain_sem, gs_sem, gs_out, far_sem, near_sem, y_sem, x_sem, z_sem, first_out, y_out, x_out, z_out,
    pk1_sem, pk1_out, pk2_sem, pk2_out,
):
    dev, ma = lax.axis_index("dev"), lax.axis_index("ma")
    zh, y = dev // 4, dev % 4
    zl, x, c = ma // 8, (ma // 2) % 4, ma % 2
    z = zh * 2 + zl
    inner = (z == 1) | (z == 2)
    outer = (z == 0) | (z == 3)
    far_z = {"dev": (1 - zh) * 4 + y, "ma": (1 - zl) * 8 + x * 2 + c}
    near_z = {"dev": dev, "ma": (1 - zl) * 8 + x * 2 + c}

    def at(x_, y_, z_, c_):
        return {"dev": (z_ // 2) * 4 + y_, "ma": (z_ % 2) * 8 + x_ * 2 + c_}

    def send(src, dst, out_sem, in_sem_, device):
        pltpu.make_async_remote_copy(src, dst, out_sem, in_sem_, device_id=device, device_id_type=MESH).start()

    def done(ref, sem):
        pltpu.make_async_copy(ref, ref, sem).wait()

    def load(t):
        return pltpu.make_async_copy(w_ref.at[t // 2, pl.ds((1 - t % 2) * FEATS, FEATS), :], xb.at[t], in_sem.at[t])

    load_rot = pltpu.make_async_copy(rot_ref, rv, rot_sem)
    load_gain = pltpu.make_async_copy(gain_ref, gv, gain_sem)

    for n in range(CHUNKS):
        load(n // 2 + (n % 2) * LATE).start()
    load_rot.start()
    load_gain.start()

    barrier = pltpu.get_barrier_semaphore()
    for step in range(1, 16):
        pl.semaphore_signal(barrier, inc=1, device_id={"dev": dev, "ma": (ma + step) % 16}, device_id_type=MESH)
    for step in range(1, 8):
        pl.semaphore_signal(barrier, inc=1, device_id={"dev": (dev + step) % 8, "ma": ma}, device_id_type=MESH)
    pl.semaphore_signal(barrier, inc=1, device_id=far_z, device_id_type=MESH)

    def place(t, half):
        kept = zh == half
        early = jnp.where(kept, jnp.where(outer, 0, 3), 2)
        return jnp.where(t < LATE, jnp.where(kept, 0, 1), early)

    def sort(n):
        t = n // 2 + (n % 2) * LATE
        load(t).wait()
        rows = lax.dot_general(pm[...], xb[t], (((1,), (1,)), ((), ())), preferred_element_type=jnp.float32)
        rows = rows.astype(jnp.bfloat16).reshape(2, 4, PAIRS, 16, FEATS)
        sb[t, place(t, 0)] = rows[0]
        sb[t, place(t, 1)] = rows[1]

    def z_first(t):
        send(sb.at[t, 2], sb.at[t, jnp.where(outer, 3, 0)], first_out.at[t], far_sem.at[t], far_z)

        @pl.when(inner)
        def _():
            send(sb.at[t, 3], sb.at[t, 1], first_out.at[t], near_sem.at[t], near_z)

    def z_first_relay(t):
        @pl.when(outer)
        def _():
            done(sb.at[t, 3], far_sem.at[t])
            send(sb.at[t, 3], sb.at[t, 1], first_out.at[t], near_sem.at[t], near_z)

    def along_y(t, q):
        @pl.when((t >= LATE) & (q == 0) & inner)
        def _():
            done(sb.at[t, 0], far_sem.at[t])

        @pl.when((t >= LATE) & (q == 1))
        def _():
            done(sb.at[t, 1], near_sem.at[t])

        pltpu.make_async_copy(sb.at[t, q, y], yb.at[t, q, y], y_sem.at[t * 2 + q]).start()
        for step in (2, 1, 3):
            far = (y + step) % 4
            send(sb.at[t, q, far], yb.at[t, q, y], y_out.at[t], y_sem.at[t * 2 + q], at(x, far, z, c))

    def along_x(t, q):
        layer, core = t // 2, 1 - t % 2
        sent, sem = x_out.at[t], x_sem.at[layer * 2 + q]
        done(yb.at[t, q], y_sem.at[t * 2 + q])
        late = jnp.where(q == 1, 3, jnp.where(outer, 1, 2))
        slot = jnp.where(t < LATE, late, jnp.where(outer, 1 - q, q))
        target = gb.at[layer, slot, x * 2 + c]
        for step in (2, 1, 3):
            far = (x + step) % 4
            send(yb.at[t, q, far], target, sent, sem, at(far, y, z, core))

        @pl.when(core != c)
        def _():
            send(yb.at[t, q, x], target, sent, sem, at(x, y, z, 1 - c))

        @pl.when(core == c)
        def _():
            pltpu.make_async_copy(yb.at[t, q, x], target, sem).start()

    def mine(t, stage):
        @pl.when(t % 2 != c)
        def _():
            stage(t // 2)

    def z_last(layer, q):
        done(gb.at[layer, 2 + q], x_sem.at[layer * 2 + q])

        @pl.when(q == 1)
        def _():
            target = gb.at[layer, jnp.where(outer, 2, 0)]
            send(gb.at[layer, 3], target, z_out.at[layer], z_sem.at[layer * 2], far_z)

        @pl.when((q == 0) & inner)
        def _():
            send(gb.at[layer, 2], gb.at[layer, 0], z_out.at[layer], z_sem.at[layer * 2 + 1], near_z)

    def z_last_relay(layer):
        @pl.when(outer)
        def _():
            done(gb.at[layer, 2], z_sem.at[layer * 2])
            send(gb.at[layer, 2], gb.at[layer, 1], z_out.at[layer], z_sem.at[layer * 2 + 1], near_z)

    def finish(layer, late):
        if late:
            done(gb.at[layer, 0], z_sem.at[layer * 2 + 1])

            @pl.when(inner)
            def _():
                done(gb.at[layer, 1], z_sem.at[layer * 2])

        else:
            done(gb.at[layer, 0], x_sem.at[layer * 2])
            done(gb.at[layer, 1], x_sem.at[layer * 2 + 1])

        @pl.when(layer != (LATE // 2 if late else LAYERS) - 1)
        def _():
            serve(gb, rm, gv, layer, out_ref, layer)

    def first_send(n):
        @pl.when(n % 2 == 0)
        def _():
            along_y(n // 2, 0)
            along_y(n // 2, 1)

        @pl.when(n % 2 == 1)
        def _():
            z_first(LATE + n // 2)

    def start(n, carry):
        sort(n)
        first_send(n - 1)
        return carry

    sort_matrix(pm)
    sort(0)
    pl.semaphore_wait(barrier, 23)
    lax.fori_loop(1, AHEAD, start, 0)
    load_gain.wait()
    load_rot.wait()

    def share_gain():
        @pl.when(ma // 2 == dev)
        def _():
            block = ma % 2
            pltpu.make_async_copy(gv, gs.at[block], gs_sem.at[block]).start()
            for step in range(1, 16):
                send(gv, gs.at[block], gs_out, gs_sem.at[block], {"dev": dev, "ma": (ma + step) % 16})

    def peaks(layer):
        @pl.when(layer == 0)
        def _():
            done(gs.at[0], gs_sem.at[0])
            done(gs.at[1], gs_sem.at[1])

        lane = lax.broadcasted_iota(jnp.int32, (192, 128), 1)
        for half in range(2):
            size = None
            for core in range(2):
                rows = sb[layer * 2 + core, place(layer * 2, half)].reshape(192, FEATS).astype(jnp.float32)
                rows = jnp.abs(rows * gs[1 - core, pl.ds(layer, 1), :])
                rows = jnp.maximum(rows[:, :128], rows[:, 128:])
                size = rows if size is None else jnp.maximum(size, rows)
            top = jnp.max(size, axis=1, keepdims=True)
            part = slice(half * 192, (half + 1) * 192)
            pt[part, :] = jnp.where(lane == layer, top, pt[part, :])

        @pl.when(layer == LAYERS - 1)
        def _():
            for block in range(3):
                lanes = slice(block * 128, (block + 1) * 128)
                pt2[:, lanes] = jnp.transpose(pt[lanes, :])[0:LAYERS, :]

    def split_peaks():
        line = pt2[...]
        for group in range(8):
            part = pltpu.roll(line, COLS - group * PIECE, 1) if group else line
            pk0[group] = part[:, 0:128].astype(jnp.bfloat16)

    def send_peaks():
        pltpu.make_async_copy(pk0.at[dev], pk1.at[dev], pk1_sem).start()
        for step in range(1, 8):
            to = (dev + step) % 8
            send(pk0.at[to], pk1.at[dev], pk1_out, pk1_sem, {"dev": to, "ma": ma})

    def group_peaks():
        done(pk1, pk1_sem)
        pk2[...] = jnp.max(pk1[...].astype(jnp.float32), axis=0).astype(jnp.bfloat16)

    def spread_peaks():
        pltpu.make_async_copy(pk2, pk3.at[8 + ma % 8], pk2_sem).start()
        for step in range(1, 16):
            to = (ma + step) % 16
            place = jnp.where(to // 8 == zl, 8, 0) + ma % 8
            send(pk2, pk3.at[place], pk2_out, pk2_sem, {"dev": dev, "ma": to})

    def close(t):
        done(sb.at[t, 0:2, 0:3], y_out.at[t])

        @pl.when(t >= LATE)
        def _():
            done(sb.at[t, 2:4], first_out.at[t])

        @pl.when(t % 2 != c)
        def _():
            done(yb.at[t, :, 0:3], x_out.at[t])

        @pl.when(t % 2 == c)
        def _():
            done(yb.at[t], x_out.at[t])

    def turn(i, carry):
        def halves(at_step, stage, first, last):
            v = i - at_step

            @pl.when((v >= first) & (v < last))
            def _():
                stage(v // 2, v % 2)

        def chunks(at_step, stage, first, last):
            v = i - at_step

            @pl.when((v >= 2 * first) & (v < 2 * last) & (v % 2 == 0))
            def _():
                stage(v // 2)

        halves(0, along_x, 0, STEPS)
        pl.when(i <= CHUNKS - AHEAD)(lambda: first_send(i + AHEAD - 1))
        halves(-LEAD, along_y, 2 * LATE, STEPS)
        chunks(Z_FIRST_RELAY, lambda j: z_first_relay(LATE + j), 0, CHUNKS - LATE)
        halves(Z_LAST, lambda t, q: mine(t, lambda layer: z_last(layer, q)), 0, 2 * LATE)
        chunks(Z_LAST_RELAY, lambda t: mine(t, z_last_relay), 0, LATE)

        @pl.when(i < CHUNKS - AHEAD)
        def _():
            sort(i + AHEAD)

        chunks(FINISH_LATE, lambda t: mine(t, lambda layer: finish(layer, True)), 0, LATE)
        chunks(FINISH, lambda j: mine(LATE + j, lambda layer: finish(layer, False)), 0, CHUNKS - LATE)

        @pl.when((i >= PEAKS_FROM) & (i < PEAKS_FROM + LAYERS))
        def _():
            peaks(i - PEAKS_FROM)

        pl.when(i == PEAKS_SEND - 1)(split_peaks)
        pl.when(i == PEAKS_SEND)(send_peaks)
        pl.when(i == PEAKS_GROUP)(group_peaks)
        pl.when(i == PEAKS_SPREAD)(spread_peaks)

        chunks(CLOSE, close, 0, CHUNKS)
        pl.when(i == SHARE)(share_gain)
        pl.when(i == MATRIX)(lambda: order_matrix(rv, rm, zl))

        return carry

    lax.fori_loop(0, END, turn, 0)

    def close_layer(layer, carry):
        @pl.when(layer < LATE // 2)
        def _():
            done(gb.at[layer, 2:4], z_out.at[layer])

        return carry

    lax.fori_loop(0, LAYERS, close_layer, 0)

    @pl.when(ma // 2 == dev)
    def _():
        done(gs.at[0:15], gs_out)

    done(pk1.at[0:7], pk1_out)
    done(pk3.at[0:15], pk2_out)
    done(pk3, pk2_sem)


def serve_peaks(pk3, rm, peak):
    lane = lax.broadcasted_iota(jnp.int32, (LAYERS, 128), 1)
    for pair in range(PAIRS):
        lines = []
        for half in range(2):
            line = jnp.zeros((LAYERS, 128), jnp.float32)
            for piece in range(8):
                shift = (piece - pair) * 16 % 128
                part = pk3[half * 8 + piece].astype(jnp.float32)
                part = pltpu.roll(part, shift, 1) if shift else part
                line = jnp.where((lane >= piece * 16) & (lane < piece * 16 + 16), part, line)
            lines.append(line)
        line = jnp.concatenate(lines, axis=1).astype(jnp.bfloat16)
        peak[:, pair * 256 : (pair + 1) * 256] = lax.dot_general(
            line, rm[pair // 2], (((1,), (1,)), ((), ())), preferred_element_type=jnp.float32
        )


def write_out(tiles_ref, pk3, gb, rm, gv, q_ref, k_ref, v_ref, row_ref, last, peak, sem):
    copies = []

    def copy(src, dst):
        copies.append(pltpu.make_async_copy(src, dst, sem.at[len(copies)]))
        copies[-1].start()

    def tiles(src, layers):
        for out, first, count in ((q_ref, 0, 512), (k_ref, 512, 128), (v_ref, 640, 128)):
            copy(src.at[:, pl.ds(first, count)], out.at[layers])

    half = LATE // 2
    for layers in (pl.ds(0, half - 1), pl.ds(half, LAYERS - half - 1)):
        tiles(tiles_ref.at[layers], layers)
    for place, layer in enumerate((half - 1, LAYERS - 1)):
        serve(gb, rm, gv, layer, last, place)
        tiles(last.at[pl.ds(place, 1)], pl.ds(layer, 1))
    serve_peaks(pk3, rm, peak)
    copy(peak, row_ref)
    for waited in copies:
        waited.wait()


def shards(joined_weight, norm_gain, rotary_order):
    dma = pltpu.SemaphoreType.DMA
    bf16, f32 = jnp.bfloat16, jnp.float32
    hbm = pl.BlockSpec(memory_space=pltpu.HBM)
    vmem = pl.BlockSpec(memory_space=pltpu.VMEM)
    moved = pl.pallas_call(
        kernel,
        name="relayout",
        out_shape=(
            jax.ShapeDtypeStruct((LAYERS, 768, FEATS), bf16),
            jax.ShapeDtypeStruct((16, LAYERS, 128), bf16),
            jax.ShapeDtypeStruct((LAYERS, 4, 8, PAIRS, 16, FEATS), bf16),
            jax.ShapeDtypeStruct((2, 256, 256), bf16),
            jax.ShapeDtypeStruct((LAYERS, FEATS), f32),
        ),
        in_specs=[hbm, hbm, hbm],
        out_specs=(vmem,) * 5,
        scratch_shapes=[
            pltpu.VMEM((1, 128), jnp.int32),
            pltpu.VMEM((15, LAYERS, FEATS), f32),
            pltpu.VMEM((CHUNKS, FEATS, COLS), bf16),
            pltpu.VMEM((CHUNKS, 4, 4, PAIRS, 16, FEATS), bf16),
            pltpu.VMEM((CHUNKS, 2, 4, PAIRS, 16, FEATS), bf16),
            pltpu.VMEM((COLS, 128), f32),
            pltpu.VMEM((LAYERS, COLS), f32),
            pltpu.VMEM((8, LAYERS, 128), bf16),
            pltpu.VMEM((8, LAYERS, 128), bf16),
            pltpu.VMEM((LAYERS, 128), bf16),
            pltpu.VMEM((COLS, COLS), bf16),
            dma((CHUNKS,)),
            dma,
            dma,
            dma((2,)),
            dma,
            dma((CHUNKS,)),
            dma((CHUNKS,)),
            dma((CHUNKS * 2,)),
            dma((LAYERS * 2,)),
            dma((LAYERS * 2,)),
            dma((CHUNKS,)),
            dma((CHUNKS,)),
            dma((CHUNKS,)),
            dma((LAYERS,)),
            dma,
            dma,
            dma,
            dma,
        ],
        compiler_params=pltpu.CompilerParams(collective_id=0, has_side_effects=True, vmem_limit_bytes=40 * 2**20),
    )(*(pltpu.with_memory_space_constraint(a, pltpu.HBM) for a in (rotary_order.reshape(1, 128), norm_gain, joined_weight)))
    return pl.pallas_call(
        write_out,
        name="write_out",
        out_shape=(
            jax.ShapeDtypeStruct((LAYERS, 512, FEATS), bf16),
            jax.ShapeDtypeStruct((LAYERS, 128, FEATS), bf16),
            jax.ShapeDtypeStruct((LAYERS, 128, FEATS), bf16),
            jax.ShapeDtypeStruct((LAYERS, 768), f32),
        ),
        in_specs=[vmem] * 5,
        out_specs=(hbm, hbm, hbm, hbm),
        scratch_shapes=[pltpu.VMEM((2, 768, FEATS), bf16), pltpu.VMEM((LAYERS, 768), f32), dma((13,))],
        compiler_params=pltpu.CompilerParams(vmem_limit_bytes=4 * 2**20),
    )(*moved)


def solution(mesh):
    placed = (P(None, "dev", "ma"), P(None, "ma"), P())
    tiles = P(None, "dev", "ma")
    return jax.shard_map(shards, mesh=mesh, in_specs=placed, out_specs=(tiles, tiles, tiles, P(None, "dev")), check_vma=False)
```

```python
import jax
import jax.numpy as jnp
from jax import lax
from jax.experimental import pallas as pl
from jax.experimental.pallas import tpu as pltpu
from jax.sharding import PartitionSpec as P

LAYERS = 8
CHUNKS = 16
FEATS = 256
COLS = 384
PIECE = 48
PAIRS = 3
LATE = 8
AHEAD = 10
LEAD = 6
SHARE, MATRIX, CLOSE = 0, 2, 5
STEPS = 2 * CHUNKS
Z_LAST, Z_LAST_RELAY, Z_FIRST_RELAY, FINISH_LATE, FINISH = 7, 17, 2, 22, 21
PEAKS_FROM, PEAKS_SEND, PEAKS_GROUP, PEAKS_SPREAD = 6, 15, 27, 28
END = max(FINISH, FINISH_LATE) + 15
MESH = pl.DeviceIdType.MESH


def sort_matrix(pm_ref):
    row = lax.broadcasted_iota(jnp.int32, (COLS, 128), 0)
    lane = lax.broadcasted_iota(jnp.int32, (COLS, 128), 1)
    g = (row * 1366) >> 16
    rest = row - g * PIECE
    s, dd = rest >> 3, rest & 7
    head = jnp.where(s < 4, g * 4 + s, 32 + (s - 4) * 8 + g)
    column = dd * PIECE + head
    for block in range(COLS // 128):
        pm_ref[:, block * 128 : (block + 1) * 128] = jnp.where(column == lane + block * 128, 1.0, 0.0).astype(jnp.bfloat16)


def order_matrix(rot_ref, rm_ref, zl):
    turned = jnp.transpose(jnp.broadcast_to(rot_ref[0:1, :], (128, 128)))
    plain = lax.broadcasted_iota(jnp.int32, (128, 128), 0)
    lane = lax.broadcasted_iota(jnp.int32, (128, 128), 1)

    def hot(stored, s2, block):
        piece = stored >> 3
        half = piece >> 3
        slot = jnp.where(zl == 1, half, 1 - half)
        column = slot * 128 + (piece & 7) * 16 + s2 * 8 + (stored & 7)
        return jnp.where(column == lane + block * 128, 1.0, 0.0).astype(jnp.bfloat16)

    for block in range(2):
        lanes = slice(block * 128, (block + 1) * 128)
        key = hot(turned, 0, block)
        rm_ref[0, 0:128, lanes] = key
        rm_ref[1, 0:128, lanes] = key
        rm_ref[0, 128:256, lanes] = hot(turned, 1, block)
        rm_ref[1, 128:256, lanes] = hot(plain, 1, block)


def serve(gb, rm, gv, layer, out_ref, place):
    gain = gv[pl.ds(layer, 1), :]
    for pair in range(PAIRS):
        arrived = gb[layer, 0:2, :, pair].reshape(256, FEATS)
        rows = jnp.dot(rm[pair // 2], arrived, preferred_element_type=jnp.float32) * gain
        out_ref[place, pair * 256 : (pair + 1) * 256, :] = rows.astype(jnp.bfloat16)


def kernel(
    rot_ref, gain_ref, w_ref, out_ref, pk3, gb, rm, gv,
    rv, gs, xb, sb, yb, pt, pt2, pk0, pk1, pk2, pm,
    in_sem, rot_sem, gain_sem, gs_sem, gs_out, far_sem, near_sem, y_sem, x_sem, z_sem, first_out, y_out, x_out, z_out,
    pk1_sem, pk1_out, pk2_sem, pk2_out,
):
    dev, ma = lax.axis_index("dev"), lax.axis_index("ma")
    zh, y = dev // 4, dev % 4
    zl, x, c = ma // 8, (ma // 2) % 4, ma % 2
    z = zh * 2 + zl
    inner = (z == 1) | (z == 2)
    outer = (z == 0) | (z == 3)
    far_z = {"dev": (1 - zh) * 4 + y, "ma": (1 - zl) * 8 + x * 2 + c}
    near_z = {"dev": dev, "ma": (1 - zl) * 8 + x * 2 + c}

    def at(x_, y_, z_, c_):
        return {"dev": (z_ // 2) * 4 + y_, "ma": (z_ % 2) * 8 + x_ * 2 + c_}

    def send(src, dst, out_sem, in_sem_, device):
        pltpu.make_async_remote_copy(src, dst, out_sem, in_sem_, device_id=device, device_id_type=MESH).start()

    def done(ref, sem):
        pltpu.make_async_copy(ref, ref, sem).wait()

    def load(t):
        return pltpu.make_async_copy(w_ref.at[t // 2, pl.ds((1 - t % 2) * FEATS, FEATS), :], xb.at[t], in_sem.at[t])

    load_rot = pltpu.make_async_copy(rot_ref, rv, rot_sem)
    load_gain = pltpu.make_async_copy(gain_ref, gv, gain_sem)

    for n in range(CHUNKS):
        load(n // 2 + (n % 2) * LATE).start()
    load_rot.start()
    load_gain.start()

    barrier = pltpu.get_barrier_semaphore()
    for step in range(1, 16):
        pl.semaphore_signal(barrier, inc=1, device_id={"dev": dev, "ma": (ma + step) % 16}, device_id_type=MESH)
    for step in range(1, 8):
        pl.semaphore_signal(barrier, inc=1, device_id={"dev": (dev + step) % 8, "ma": ma}, device_id_type=MESH)
    pl.semaphore_signal(barrier, inc=1, device_id=far_z, device_id_type=MESH)

    def place(t, half):
        kept = zh == half
        early = jnp.where(kept, jnp.where(outer, 0, 3), 2)
        return jnp.where(t < LATE, jnp.where(kept, 0, 1), early)

    def sort(n):
        t = n // 2 + (n % 2) * LATE
        load(t).wait()
        rows = lax.dot_general(pm[...], xb[t], (((1,), (1,)), ((), ())), preferred_element_type=jnp.float32)
        rows = rows.astype(jnp.bfloat16).reshape(2, 4, PAIRS, 16, FEATS)
        sb[t, place(t, 0)] = rows[0]
        sb[t, place(t, 1)] = rows[1]

    def z_first(t):
        send(sb.at[t, 2], sb.at[t, jnp.where(outer, 3, 0)], first_out.at[t], far_sem.at[t], far_z)

        @pl.when(inner)
        def _():
            send(sb.at[t, 3], sb.at[t, 1], first_out.at[t], near_sem.at[t], near_z)

    def z_first_relay(t):
        @pl.when(outer)
        def _():
            done(sb.at[t, 3], far_sem.at[t])
            send(sb.at[t, 3], sb.at[t, 1], first_out.at[t], near_sem.at[t], near_z)

    def along_y(t, q):
        @pl.when((t >= LATE) & (q == 0) & inner)
        def _():
            done(sb.at[t, 0], far_sem.at[t])

        @pl.when((t >= LATE) & (q == 1))
        def _():
            done(sb.at[t, 1], near_sem.at[t])

        pltpu.make_async_copy(sb.at[t, q, y], yb.at[t, q, y], y_sem.at[t * 2 + q]).start()
        for step in (2, 1, 3):
            far = (y + step) % 4
            send(sb.at[t, q, far], yb.at[t, q, y], y_out.at[t], y_sem.at[t * 2 + q], at(x, far, z, c))

    def along_x(t, q):
        layer, core = t // 2, 1 - t % 2
        sent, sem = x_out.at[t], x_sem.at[layer * 2 + q]
        done(yb.at[t, q], y_sem.at[t * 2 + q])
        late = jnp.where(q == 1, 3, jnp.where(outer, 1, 2))
        slot = jnp.where(t < LATE, late, jnp.where(outer, 1 - q, q))
        target = gb.at[layer, slot, x * 2 + c]
        for step in (2, 1, 3):
            far = (x + step) % 4
            send(yb.at[t, q, far], target, sent, sem, at(far, y, z, core))

        @pl.when(core != c)
        def _():
            send(yb.at[t, q, x], target, sent, sem, at(x, y, z, 1 - c))

        @pl.when(core == c)
        def _():
            pltpu.make_async_copy(yb.at[t, q, x], target, sem).start()

    def mine(t, stage):
        @pl.when(t % 2 != c)
        def _():
            stage(t // 2)

    def z_last(layer, q):
        done(gb.at[layer, 2 + q], x_sem.at[layer * 2 + q])

        @pl.when(q == 1)
        def _():
            target = gb.at[layer, jnp.where(outer, 2, 0)]
            send(gb.at[layer, 3], target, z_out.at[layer], z_sem.at[layer * 2], far_z)

        @pl.when((q == 0) & inner)
        def _():
            send(gb.at[layer, 2], gb.at[layer, 0], z_out.at[layer], z_sem.at[layer * 2 + 1], near_z)

    def z_last_relay(layer):
        @pl.when(outer)
        def _():
            done(gb.at[layer, 2], z_sem.at[layer * 2])
            send(gb.at[layer, 2], gb.at[layer, 1], z_out.at[layer], z_sem.at[layer * 2 + 1], near_z)

    def finish(layer, late):
        if late:
            done(gb.at[layer, 0], z_sem.at[layer * 2 + 1])

            @pl.when(inner)
            def _():
                done(gb.at[layer, 1], z_sem.at[layer * 2])

        else:
            done(gb.at[layer, 0], x_sem.at[layer * 2])
            done(gb.at[layer, 1], x_sem.at[layer * 2 + 1])

        @pl.when(layer != (LATE // 2 if late else LAYERS) - 1)
        def _():
            serve(gb, rm, gv, layer, out_ref, layer)

    def first_send(n):
        @pl.when(n % 2 == 0)
        def _():
            along_y(n // 2, 0)
            along_y(n // 2, 1)

        @pl.when(n % 2 == 1)
        def _():
            z_first(LATE + n // 2)

    def start(n, carry):
        sort(n)
        first_send(n - 1)
        return carry

    sort_matrix(pm)
    sort(0)
    pl.semaphore_wait(barrier, 23)
    lax.fori_loop(1, AHEAD, start, 0)
    load_gain.wait()
    load_rot.wait()

    def share_gain():
        @pl.when(ma // 2 == dev)
        def _():
            block = ma % 2
            pltpu.make_async_copy(gv, gs.at[block], gs_sem.at[block]).start()
            for step in range(1, 16):
                send(gv, gs.at[block], gs_out, gs_sem.at[block], {"dev": dev, "ma": (ma + step) % 16})

    def peaks(layer):
        @pl.when(layer == 0)
        def _():
            done(gs.at[0], gs_sem.at[0])
            done(gs.at[1], gs_sem.at[1])

        lane = lax.broadcasted_iota(jnp.int32, (192, 128), 1)
        for half in range(2):
            size = None
            for core in range(2):
                rows = sb[layer * 2 + core, place(layer * 2, half)].reshape(192, FEATS).astype(jnp.float32)
                rows = jnp.abs(rows * gs[1 - core, pl.ds(layer, 1), :])
                rows = jnp.maximum(rows[:, :128], rows[:, 128:])
                size = rows if size is None else jnp.maximum(size, rows)
            top = jnp.max(size, axis=1, keepdims=True)
            part = slice(half * 192, (half + 1) * 192)
            pt[part, :] = jnp.where(lane == layer, top, pt[part, :])

        @pl.when(layer == LAYERS - 1)
        def _():
            for block in range(3):
                lanes = slice(block * 128, (block + 1) * 128)
                pt2[:, lanes] = jnp.transpose(pt[lanes, :])[0:LAYERS, :]

    def split_peaks():
        line = pt2[...]
        for group in range(8):
            part = pltpu.roll(line, COLS - group * PIECE, 1) if group else line
            pk0[group] = part[:, 0:128].astype(jnp.bfloat16)

    def send_peaks():
        pltpu.make_async_copy(pk0.at[dev], pk1.at[dev], pk1_sem).start()
        for step in range(1, 8):
            to = (dev + step) % 8
            send(pk0.at[to], pk1.at[dev], pk1_out, pk1_sem, {"dev": to, "ma": ma})

    def group_peaks():
        done(pk1, pk1_sem)
        pk2[...] = jnp.max(pk1[...].astype(jnp.float32), axis=0).astype(jnp.bfloat16)

    def spread_peaks():
        pltpu.make_async_copy(pk2, pk3.at[8 + ma % 8], pk2_sem).start()
        for step in range(1, 16):
            to = (ma + step) % 16
            place = jnp.where(to // 8 == zl, 8, 0) + ma % 8
            send(pk2, pk3.at[place], pk2_out, pk2_sem, {"dev": dev, "ma": to})

    def close(t):
        done(sb.at[t, 0:2, 0:3], y_out.at[t])

        @pl.when(t >= LATE)
        def _():
            done(sb.at[t, 2:4], first_out.at[t])

        @pl.when(t % 2 != c)
        def _():
            done(yb.at[t, :, 0:3], x_out.at[t])

        @pl.when(t % 2 == c)
        def _():
            done(yb.at[t], x_out.at[t])

    def turn(i, carry):
        def halves(at_step, stage, first, last):
            v = i - at_step

            @pl.when((v >= first) & (v < last))
            def _():
                stage(v // 2, v % 2)

        def chunks(at_step, stage, first, last):
            v = i - at_step

            @pl.when((v >= 2 * first) & (v < 2 * last) & (v % 2 == 0))
            def _():
                stage(v // 2)

        halves(0, along_x, 0, STEPS)
        pl.when(i <= CHUNKS - AHEAD)(lambda: first_send(i + AHEAD - 1))
        halves(-LEAD, along_y, 2 * LATE, STEPS)
        chunks(Z_FIRST_RELAY, lambda j: z_first_relay(LATE + j), 0, CHUNKS - LATE)
        halves(Z_LAST, lambda t, q: mine(t, lambda layer: z_last(layer, q)), 0, 2 * LATE)
        chunks(Z_LAST_RELAY, lambda t: mine(t, z_last_relay), 0, LATE)

        @pl.when(i < CHUNKS - AHEAD)
        def _():
            sort(i + AHEAD)

        chunks(FINISH_LATE, lambda t: mine(t, lambda layer: finish(layer, True)), 0, LATE)
        chunks(FINISH, lambda j: mine(LATE + j, lambda layer: finish(layer, False)), 0, CHUNKS - LATE)

        @pl.when((i >= PEAKS_FROM) & (i < PEAKS_FROM + LAYERS))
        def _():
            peaks(i - PEAKS_FROM)

        pl.when(i == PEAKS_SEND - 1)(split_peaks)
        pl.when(i == PEAKS_SEND)(send_peaks)
        pl.when(i == PEAKS_GROUP)(group_peaks)
        pl.when(i == PEAKS_SPREAD)(spread_peaks)

        chunks(CLOSE, close, 0, CHUNKS)
        pl.when(i == SHARE)(share_gain)
        pl.when(i == MATRIX)(lambda: order_matrix(rv, rm, zl))

        return carry

    lax.fori_loop(0, END, turn, 0)

    def close_layer(layer, carry):
        @pl.when(layer < LATE // 2)
        def _():
            done(gb.at[layer, 2:4], z_out.at[layer])

        return carry

    lax.fori_loop(0, LAYERS, close_layer, 0)

    @pl.when(ma // 2 == dev)
    def _():
        done(gs.at[0:15], gs_out)

    done(pk1.at[0:7], pk1_out)
    done(pk3.at[0:15], pk2_out)
    done(pk3, pk2_sem)


def serve_peaks(pk3, rm, peak):
    lane = lax.broadcasted_iota(jnp.int32, (LAYERS, 128), 1)
    for pair in range(PAIRS):
        lines = []
        for half in range(2):
            line = jnp.zeros((LAYERS, 128), jnp.float32)
            for piece in range(8):
                shift = (piece - pair) * 16 % 128
                part = pk3[half * 8 + piece].astype(jnp.float32)
                part = pltpu.roll(part, shift, 1) if shift else part
                line = jnp.where((lane >= piece * 16) & (lane < piece * 16 + 16), part, line)
            lines.append(line)
        line = jnp.concatenate(lines, axis=1).astype(jnp.bfloat16)
        peak[:, pair * 256 : (pair + 1) * 256] = lax.dot_general(
            line, rm[pair // 2], (((1,), (1,)), ((), ())), preferred_element_type=jnp.float32
        )


def write_out(tiles_ref, pk3, gb, rm, gv, q_ref, k_ref, v_ref, row_ref, last, peak, sem):
    copies = []

    def copy(src, dst):
        copies.append(pltpu.make_async_copy(src, dst, sem.at[len(copies)]))
        copies[-1].start()

    def tiles(src, layers):
        for out, first, count in ((q_ref, 0, 512), (k_ref, 512, 128), (v_ref, 640, 128)):
            copy(src.at[:, pl.ds(first, count)], out.at[layers])

    half = LATE // 2
    for layers in (pl.ds(0, half - 1), pl.ds(half, LAYERS - half - 1)):
        tiles(tiles_ref.at[layers], layers)
    for place, layer in enumerate((half - 1, LAYERS - 1)):
        serve(gb, rm, gv, layer, last, place)
        tiles(last.at[pl.ds(place, 1)], pl.ds(layer, 1))
    serve_peaks(pk3, rm, peak)
    copy(peak, row_ref)
    for waited in copies:
        waited.wait()


def shards(joined_weight, norm_gain, rotary_order):
    dma = pltpu.SemaphoreType.DMA
    bf16, f32 = jnp.bfloat16, jnp.float32
    hbm = pl.BlockSpec(memory_space=pltpu.HBM)
    vmem = pl.BlockSpec(memory_space=pltpu.VMEM)
    moved = pl.pallas_call(
        kernel,
        name="relayout",
        out_shape=(
            jax.ShapeDtypeStruct((LAYERS, 768, FEATS), bf16),
            jax.ShapeDtypeStruct((16, LAYERS, 128), bf16),
            jax.ShapeDtypeStruct((LAYERS, 4, 8, PAIRS, 16, FEATS), bf16),
            jax.ShapeDtypeStruct((2, 256, 256), bf16),
            jax.ShapeDtypeStruct((LAYERS, FEATS), f32),
        ),
        in_specs=[hbm, hbm, hbm],
        out_specs=(vmem,) * 5,
        scratch_shapes=[
            pltpu.VMEM((1, 128), jnp.int32),
            pltpu.VMEM((15, LAYERS, FEATS), f32),
            pltpu.VMEM((CHUNKS, FEATS, COLS), bf16),
            pltpu.VMEM((CHUNKS, 4, 4, PAIRS, 16, FEATS), bf16),
            pltpu.VMEM((CHUNKS, 2, 4, PAIRS, 16, FEATS), bf16),
            pltpu.VMEM((COLS, 128), f32),
            pltpu.VMEM((LAYERS, COLS), f32),
            pltpu.VMEM((8, LAYERS, 128), bf16),
            pltpu.VMEM((8, LAYERS, 128), bf16),
            pltpu.VMEM((LAYERS, 128), bf16),
            pltpu.VMEM((COLS, COLS), bf16),
            dma((CHUNKS,)),
            dma,
            dma,
            dma((2,)),
            dma,
            dma((CHUNKS,)),
            dma((CHUNKS,)),
            dma((CHUNKS * 2,)),
            dma((LAYERS * 2,)),
            dma((LAYERS * 2,)),
            dma((CHUNKS,)),
            dma((CHUNKS,)),
            dma((CHUNKS,)),
            dma((LAYERS,)),
            dma,
            dma,
            dma,
            dma,
        ],
        compiler_params=pltpu.CompilerParams(collective_id=0, has_side_effects=True, vmem_limit_bytes=40 * 2**20),
    )(*(pltpu.with_memory_space_constraint(a, pltpu.HBM) for a in (rotary_order.reshape(1, 128), norm_gain, joined_weight)))
    return pl.pallas_call(
        write_out,
        name="write_out",
        out_shape=(
            jax.ShapeDtypeStruct((LAYERS, 512, FEATS), bf16),
            jax.ShapeDtypeStruct((LAYERS, 128, FEATS), bf16),
            jax.ShapeDtypeStruct((LAYERS, 128, FEATS), bf16),
            jax.ShapeDtypeStruct((LAYERS, 768), f32),
        ),
        in_specs=[vmem] * 5,
        out_specs=(hbm, hbm, hbm, hbm),
        scratch_shapes=[pltpu.VMEM((2, 768, FEATS), bf16), pltpu.VMEM((LAYERS, 768), f32), dma((13,))],
        compiler_params=pltpu.CompilerParams(vmem_limit_bytes=4 * 2**20),
    )(*moved)


def solution(mesh):
    placed = (P(None, "dev", "ma"), P(None, "ma"), P())
    tiles = P(None, "dev", "ma")
    return jax.shard_map(shards, mesh=mesh, in_specs=placed, out_specs=(tiles, tiles, tiles, P(None, "dev")), check_vma=False)
```

```python
import jax
import jax.numpy as jnp
from jax import lax
from jax.experimental import pallas as pl
from jax.experimental.pallas import tpu as pltpu
from jax.sharding import PartitionSpec as P

LAYERS = 8
CHUNKS = 16
FEATS = 256
COLS = 384
PIECE = 48
PAIRS = 3
LATE = 8
AHEAD = 10
LEAD = 5
SHARE, MATRIX, CLOSE = 0, 2, 5
STEPS = 2 * CHUNKS
Z_LAST, Z_LAST_RELAY, Z_FIRST_RELAY, FINISH_LATE, FINISH = 7, 16, 2, 22, 21
PEAKS_FROM, PEAKS_SEND, PEAKS_GROUP, PEAKS_SPREAD = 6, 15, 27, 28
END = max(FINISH, FINISH_LATE) + 15
MESH = pl.DeviceIdType.MESH


def sort_matrix(pm_ref):
    row = lax.broadcasted_iota(jnp.int32, (COLS, 128), 0)
    lane = lax.broadcasted_iota(jnp.int32, (COLS, 128), 1)
    g = (row * 1366) >> 16
    rest = row - g * PIECE
    s, dd = rest >> 3, rest & 7
    head = jnp.where(s < 4, g * 4 + s, 32 + (s - 4) * 8 + g)
    column = dd * PIECE + head
    for block in range(COLS // 128):
        pm_ref[:, block * 128 : (block + 1) * 128] = jnp.where(column == lane + block * 128, 1.0, 0.0).astype(jnp.bfloat16)


def order_matrix(rot_ref, rm_ref, zl):
    turned = jnp.transpose(jnp.broadcast_to(rot_ref[0:1, :], (128, 128)))
    plain = lax.broadcasted_iota(jnp.int32, (128, 128), 0)
    lane = lax.broadcasted_iota(jnp.int32, (128, 128), 1)

    def hot(stored, s2, block):
        piece = stored >> 3
        half = piece >> 3
        slot = jnp.where(zl == 1, half, 1 - half)
        column = slot * 128 + (piece & 7) * 16 + s2 * 8 + (stored & 7)
        return jnp.where(column == lane + block * 128, 1.0, 0.0).astype(jnp.bfloat16)

    for block in range(2):
        lanes = slice(block * 128, (block + 1) * 128)
        key = hot(turned, 0, block)
        rm_ref[0, 0:128, lanes] = key
        rm_ref[1, 0:128, lanes] = key
        rm_ref[0, 128:256, lanes] = hot(turned, 1, block)
        rm_ref[1, 128:256, lanes] = hot(plain, 1, block)


def serve(gb, rm, gv, layer, out_ref, place):
    gain = gv[pl.ds(layer, 1), :]
    for pair in range(PAIRS):
        arrived = gb[layer, 0:2, :, pair].reshape(256, FEATS)
        rows = jnp.dot(rm[pair // 2], arrived, preferred_element_type=jnp.float32) * gain
        out_ref[place, pair * 256 : (pair + 1) * 256, :] = rows.astype(jnp.bfloat16)


def kernel(
    rot_ref, gain_ref, w_ref, out_ref, pk3, gb, rm, gv,
    rv, gs, xb, sb, yb, pt, pt2, pk0, pk1, pk2, pm,
    in_sem, rot_sem, gain_sem, gs_sem, gs_out, far_sem, near_sem, y_sem, x_sem, z_sem, first_out, y_out, x_out, z_out,
    pk1_sem, pk1_out, pk2_sem, pk2_out,
):
    dev, ma = lax.axis_index("dev"), lax.axis_index("ma")
    zh, y = dev // 4, dev % 4
    zl, x, c = ma // 8, (ma // 2) % 4, ma % 2
    z = zh * 2 + zl
    inner = (z == 1) | (z == 2)
    outer = (z == 0) | (z == 3)
    far_z = {"dev": (1 - zh) * 4 + y, "ma": (1 - zl) * 8 + x * 2 + c}
    near_z = {"dev": dev, "ma": (1 - zl) * 8 + x * 2 + c}

    def at(x_, y_, z_, c_):
        return {"dev": (z_ // 2) * 4 + y_, "ma": (z_ % 2) * 8 + x_ * 2 + c_}

    def send(src, dst, out_sem, in_sem_, device):
        pltpu.make_async_remote_copy(src, dst, out_sem, in_sem_, device_id=device, device_id_type=MESH).start()

    def done(ref, sem):
        pltpu.make_async_copy(ref, ref, sem).wait()

    def load(t):
        return pltpu.make_async_copy(w_ref.at[t // 2, pl.ds((1 - t % 2) * FEATS, FEATS), :], xb.at[t], in_sem.at[t])

    load_rot = pltpu.make_async_copy(rot_ref, rv, rot_sem)
    load_gain = pltpu.make_async_copy(gain_ref, gv, gain_sem)

    for n in range(CHUNKS):
        load(n // 2 + (n % 2) * LATE).start()
    load_rot.start()
    load_gain.start()

    barrier = pltpu.get_barrier_semaphore()
    for step in range(1, 16):
        pl.semaphore_signal(barrier, inc=1, device_id={"dev": dev, "ma": (ma + step) % 16}, device_id_type=MESH)
    for step in range(1, 8):
        pl.semaphore_signal(barrier, inc=1, device_id={"dev": (dev + step) % 8, "ma": ma}, device_id_type=MESH)
    pl.semaphore_signal(barrier, inc=1, device_id=far_z, device_id_type=MESH)

    def place(t, half):
        kept = zh == half
        early = jnp.where(kept, jnp.where(outer, 0, 3), 2)
        return jnp.where(t < LATE, jnp.where(kept, 0, 1), early)

    def sort(n):
        t = n // 2 + (n % 2) * LATE
        load(t).wait()
        rows = lax.dot_general(pm[...], xb[t], (((1,), (1,)), ((), ())), preferred_element_type=jnp.float32)
        rows = rows.astype(jnp.bfloat16).reshape(2, 4, PAIRS, 16, FEATS)
        sb[t, place(t, 0)] = rows[0]
        sb[t, place(t, 1)] = rows[1]

    def z_first(t):
        send(sb.at[t, 2], sb.at[t, jnp.where(outer, 3, 0)], first_out.at[t], far_sem.at[t], far_z)

        @pl.when(inner)
        def _():
            send(sb.at[t, 3], sb.at[t, 1], first_out.at[t], near_sem.at[t], near_z)

    def z_first_relay(t):
        @pl.when(outer)
        def _():
            done(sb.at[t, 3], far_sem.at[t])
            send(sb.at[t, 3], sb.at[t, 1], first_out.at[t], near_sem.at[t], near_z)

    def along_y(t, q):
        @pl.when((t >= LATE) & (q == 0) & inner)
        def _():
            done(sb.at[t, 0], far_sem.at[t])

        @pl.when((t >= LATE) & (q == 1))
        def _():
            done(sb.at[t, 1], near_sem.at[t])

        pltpu.make_async_copy(sb.at[t, q, y], yb.at[t, q, y], y_sem.at[t * 2 + q]).start()
        for step in (2, 1, 3):
            far = (y + step) % 4
            send(sb.at[t, q, far], yb.at[t, q, y], y_out.at[t], y_sem.at[t * 2 + q], at(x, far, z, c))

    def along_x(t, q):
        layer, core = t // 2, 1 - t % 2
        sent, sem = x_out.at[t], x_sem.at[layer * 2 + q]
        done(yb.at[t, q], y_sem.at[t * 2 + q])
        late = jnp.where(q == 1, 3, jnp.where(outer, 1, 2))
        slot = jnp.where(t < LATE, late, jnp.where(outer, 1 - q, q))
        target = gb.at[layer, slot, x * 2 + c]
        for step in (2, 1, 3):
            far = (x + step) % 4
            send(yb.at[t, q, far], target, sent, sem, at(far, y, z, core))

        @pl.when(core != c)
        def _():
            send(yb.at[t, q, x], target, sent, sem, at(x, y, z, 1 - c))

        @pl.when(core == c)
        def _():
            pltpu.make_async_copy(yb.at[t, q, x], target, sem).start()

    def mine(t, stage):
        @pl.when(t % 2 != c)
        def _():
            stage(t // 2)

    def z_last(layer, q):
        done(gb.at[layer, 2 + q], x_sem.at[layer * 2 + q])

        @pl.when(q == 1)
        def _():
            target = gb.at[layer, jnp.where(outer, 2, 0)]
            send(gb.at[layer, 3], target, z_out.at[layer], z_sem.at[layer * 2], far_z)

        @pl.when((q == 0) & inner)
        def _():
            send(gb.at[layer, 2], gb.at[layer, 0], z_out.at[layer], z_sem.at[layer * 2 + 1], near_z)

    def z_last_relay(layer):
        @pl.when(outer)
        def _():
            done(gb.at[layer, 2], z_sem.at[layer * 2])
            send(gb.at[layer, 2], gb.at[layer, 1], z_out.at[layer], z_sem.at[layer * 2 + 1], near_z)

    def finish(layer, late):
        if late:
            done(gb.at[layer, 0], z_sem.at[layer * 2 + 1])

            @pl.when(inner)
            def _():
                done(gb.at[layer, 1], z_sem.at[layer * 2])

        else:
            done(gb.at[layer, 0], x_sem.at[layer * 2])
            done(gb.at[layer, 1], x_sem.at[layer * 2 + 1])

        @pl.when(layer != (LATE // 2 if late else LAYERS) - 1)
        def _():
            serve(gb, rm, gv, layer, out_ref, layer)

    def first_send(n):
        @pl.when(n % 2 == 0)
        def _():
            along_y(n // 2, 0)
            along_y(n // 2, 1)

        @pl.when(n % 2 == 1)
        def _():
            z_first(LATE + n // 2)

    def start(n, carry):
        sort(n)
        first_send(n - 1)
        return carry

    sort_matrix(pm)
    sort(0)
    pl.semaphore_wait(barrier, 23)
    lax.fori_loop(1, AHEAD, start, 0)
    load_gain.wait()
    load_rot.wait()

    def share_gain():
        @pl.when(ma // 2 == dev)
        def _():
            block = ma % 2
            pltpu.make_async_copy(gv, gs.at[block], gs_sem.at[block]).start()
            for step in range(1, 16):
                send(gv, gs.at[block], gs_out, gs_sem.at[block], {"dev": dev, "ma": (ma + step) % 16})

    def peaks(layer):
        @pl.when(layer == 0)
        def _():
            done(gs.at[0], gs_sem.at[0])
            done(gs.at[1], gs_sem.at[1])

        lane = lax.broadcasted_iota(jnp.int32, (192, 128), 1)
        for half in range(2):
            size = None
            for core in range(2):
                rows = sb[layer * 2 + core, place(layer * 2, half)].reshape(192, FEATS).astype(jnp.float32)
                rows = jnp.abs(rows * gs[1 - core, pl.ds(layer, 1), :])
                rows = jnp.maximum(rows[:, :128], rows[:, 128:])
                size = rows if size is None else jnp.maximum(size, rows)
            top = jnp.max(size, axis=1, keepdims=True)
            part = slice(half * 192, (half + 1) * 192)
            pt[part, :] = jnp.where(lane == layer, top, pt[part, :])

        @pl.when(layer == LAYERS - 1)
        def _():
            for block in range(3):
                lanes = slice(block * 128, (block + 1) * 128)
                pt2[:, lanes] = jnp.transpose(pt[lanes, :])[0:LAYERS, :]

    def split_peaks():
        line = pt2[...]
        for group in range(8):
            part = pltpu.roll(line, COLS - group * PIECE, 1) if group else line
            pk0[group] = part[:, 0:128].astype(jnp.bfloat16)

    def send_peaks():
        pltpu.make_async_copy(pk0.at[dev], pk1.at[dev], pk1_sem).start()
        for step in range(1, 8):
            to = (dev + step) % 8
            send(pk0.at[to], pk1.at[dev], pk1_out, pk1_sem, {"dev": to, "ma": ma})

    def group_peaks():
        done(pk1, pk1_sem)
        pk2[...] = jnp.max(pk1[...].astype(jnp.float32), axis=0).astype(jnp.bfloat16)

    def spread_peaks():
        pltpu.make_async_copy(pk2, pk3.at[8 + ma % 8], pk2_sem).start()
        for step in range(1, 16):
            to = (ma + step) % 16
            place = jnp.where(to // 8 == zl, 8, 0) + ma % 8
            send(pk2, pk3.at[place], pk2_out, pk2_sem, {"dev": dev, "ma": to})

    def close(t):
        done(sb.at[t, 0:2, 0:3], y_out.at[t])

        @pl.when(t >= LATE)
        def _():
            done(sb.at[t, 2:4], first_out.at[t])

        @pl.when(t % 2 != c)
        def _():
            done(yb.at[t, :, 0:3], x_out.at[t])

        @pl.when(t % 2 == c)
        def _():
            done(yb.at[t], x_out.at[t])

    def turn(i, carry):
        def halves(at_step, stage, first, last):
            v = i - at_step

            @pl.when((v >= first) & (v < last))
            def _():
                stage(v // 2, v % 2)

        def chunks(at_step, stage, first, last):
            v = i - at_step

            @pl.when((v >= 2 * first) & (v < 2 * last) & (v % 2 == 0))
            def _():
                stage(v // 2)

        halves(0, along_x, 0, STEPS)
        pl.when(i <= CHUNKS - AHEAD)(lambda: first_send(i + AHEAD - 1))
        halves(-LEAD, along_y, 2 * LATE, STEPS)
        chunks(Z_FIRST_RELAY, lambda j: z_first_relay(LATE + j), 0, CHUNKS - LATE)
        halves(Z_LAST, lambda t, q: mine(t, lambda layer: z_last(layer, q)), 0, 2 * LATE)
        chunks(Z_LAST_RELAY, lambda t: mine(t, z_last_relay), 0, LATE)

        @pl.when(i < CHUNKS - AHEAD)
        def _():
            sort(i + AHEAD)

        chunks(FINISH_LATE, lambda t: mine(t, lambda layer: finish(layer, True)), 0, LATE)
        chunks(FINISH, lambda j: mine(LATE + j, lambda layer: finish(layer, False)), 0, CHUNKS - LATE)

        @pl.when((i >= PEAKS_FROM) & (i < PEAKS_FROM + LAYERS))
        def _():
            peaks(i - PEAKS_FROM)

        pl.when(i == PEAKS_SEND - 1)(split_peaks)
        pl.when(i == PEAKS_SEND)(send_peaks)
        pl.when(i == PEAKS_GROUP)(group_peaks)
        pl.when(i == PEAKS_SPREAD)(spread_peaks)

        chunks(CLOSE, close, 0, CHUNKS)
        pl.when(i == SHARE)(share_gain)
        pl.when(i == MATRIX)(lambda: order_matrix(rv, rm, zl))

        return carry

    lax.fori_loop(0, END, turn, 0)

    def close_layer(layer, carry):
        @pl.when(layer < LATE // 2)
        def _():
            done(gb.at[layer, 2:4], z_out.at[layer])

        return carry

    lax.fori_loop(0, LAYERS, close_layer, 0)

    @pl.when(ma // 2 == dev)
    def _():
        done(gs.at[0:15], gs_out)

    done(pk1.at[0:7], pk1_out)
    done(pk3.at[0:15], pk2_out)
    done(pk3, pk2_sem)


def serve_peaks(pk3, rm, peak):
    lane = lax.broadcasted_iota(jnp.int32, (LAYERS, 128), 1)
    for pair in range(PAIRS):
        lines = []
        for half in range(2):
            line = jnp.zeros((LAYERS, 128), jnp.float32)
            for piece in range(8):
                shift = (piece - pair) * 16 % 128
                part = pk3[half * 8 + piece].astype(jnp.float32)
                part = pltpu.roll(part, shift, 1) if shift else part
                line = jnp.where((lane >= piece * 16) & (lane < piece * 16 + 16), part, line)
            lines.append(line)
        line = jnp.concatenate(lines, axis=1).astype(jnp.bfloat16)
        peak[:, pair * 256 : (pair + 1) * 256] = lax.dot_general(
            line, rm[pair // 2], (((1,), (1,)), ((), ())), preferred_element_type=jnp.float32
        )


def write_out(tiles_ref, pk3, gb, rm, gv, q_ref, k_ref, v_ref, row_ref, last, peak, sem):
    copies = []

    def copy(src, dst):
        copies.append(pltpu.make_async_copy(src, dst, sem.at[len(copies)]))
        copies[-1].start()

    def tiles(src, layers):
        for out, first, count in ((q_ref, 0, 512), (k_ref, 512, 128), (v_ref, 640, 128)):
            copy(src.at[:, pl.ds(first, count)], out.at[layers])

    half = LATE // 2
    for layers in (pl.ds(0, half - 1), pl.ds(half, LAYERS - half - 1)):
        tiles(tiles_ref.at[layers], layers)
    for place, layer in enumerate((half - 1, LAYERS - 1)):
        serve(gb, rm, gv, layer, last, place)
        tiles(last.at[pl.ds(place, 1)], pl.ds(layer, 1))
    serve_peaks(pk3, rm, peak)
    copy(peak, row_ref)
    for waited in copies:
        waited.wait()


def shards(joined_weight, norm_gain, rotary_order):
    dma = pltpu.SemaphoreType.DMA
    bf16, f32 = jnp.bfloat16, jnp.float32
    hbm = pl.BlockSpec(memory_space=pltpu.HBM)
    vmem = pl.BlockSpec(memory_space=pltpu.VMEM)
    moved = pl.pallas_call(
        kernel,
        name="relayout",
        out_shape=(
            jax.ShapeDtypeStruct((LAYERS, 768, FEATS), bf16),
            jax.ShapeDtypeStruct((16, LAYERS, 128), bf16),
            jax.ShapeDtypeStruct((LAYERS, 4, 8, PAIRS, 16, FEATS), bf16),
            jax.ShapeDtypeStruct((2, 256, 256), bf16),
            jax.ShapeDtypeStruct((LAYERS, FEATS), f32),
        ),
        in_specs=[hbm, hbm, hbm],
        out_specs=(vmem,) * 5,
        scratch_shapes=[
            pltpu.VMEM((1, 128), jnp.int32),
            pltpu.VMEM((15, LAYERS, FEATS), f32),
            pltpu.VMEM((CHUNKS, FEATS, COLS), bf16),
            pltpu.VMEM((CHUNKS, 4, 4, PAIRS, 16, FEATS), bf16),
            pltpu.VMEM((CHUNKS, 2, 4, PAIRS, 16, FEATS), bf16),
            pltpu.VMEM((COLS, 128), f32),
            pltpu.VMEM((LAYERS, COLS), f32),
            pltpu.VMEM((8, LAYERS, 128), bf16),
            pltpu.VMEM((8, LAYERS, 128), bf16),
            pltpu.VMEM((LAYERS, 128), bf16),
            pltpu.VMEM((COLS, COLS), bf16),
            dma((CHUNKS,)),
            dma,
            dma,
            dma((2,)),
            dma,
            dma((CHUNKS,)),
            dma((CHUNKS,)),
            dma((CHUNKS * 2,)),
            dma((LAYERS * 2,)),
            dma((LAYERS * 2,)),
            dma((CHUNKS,)),
            dma((CHUNKS,)),
            dma((CHUNKS,)),
            dma((LAYERS,)),
            dma,
            dma,
            dma,
            dma,
        ],
        compiler_params=pltpu.CompilerParams(collective_id=0, has_side_effects=True, vmem_limit_bytes=40 * 2**20),
    )(*(pltpu.with_memory_space_constraint(a, pltpu.HBM) for a in (rotary_order.reshape(1, 128), norm_gain, joined_weight)))
    return pl.pallas_call(
        write_out,
        name="write_out",
        out_shape=(
            jax.ShapeDtypeStruct((LAYERS, 512, FEATS), bf16),
            jax.ShapeDtypeStruct((LAYERS, 128, FEATS), bf16),
            jax.ShapeDtypeStruct((LAYERS, 128, FEATS), bf16),
            jax.ShapeDtypeStruct((LAYERS, 768), f32),
        ),
        in_specs=[vmem] * 5,
        out_specs=(hbm, hbm, hbm, hbm),
        scratch_shapes=[pltpu.VMEM((2, 768, FEATS), bf16), pltpu.VMEM((LAYERS, 768), f32), dma((13,))],
        compiler_params=pltpu.CompilerParams(vmem_limit_bytes=4 * 2**20),
    )(*moved)


def solution(mesh):
    placed = (P(None, "dev", "ma"), P(None, "ma"), P())
    tiles = P(None, "dev", "ma")
    return jax.shard_map(shards, mesh=mesh, in_specs=placed, out_specs=(tiles, tiles, tiles, P(None, "dev")), check_vma=False)
```
